256 devices in a mesh: dp: 32 (over z_lo, x, core), mp: 8 (over z_hi, y).
Axes of the slice: x: 4, y: 4, z: 8 (z_hi: 2, z_lo: 4; z = z_hi * 4 + z_lo), core: 2. Of those that a mesh axis runs over, the one named last changes fastest.
Arguments:
- queries: bfloat16 [24576, 1024], P('dp', 'mp'), may hold values from -3 to 3
- passages: bfloat16 [24576, 1024], P('dp', 'mp'), may hold values from -3 to 3
- positive: int32 [24576], P('dp'), may hold values from 0 to 24575
Outputs:
- grad_queries: bfloat16 [24576, 1024], P('dp', 'mp')
- grad_passages: bfloat16 [24576, 1024], P('dp', 'mp')
The draws below stay inside these ranges and needn't reach their ends.
All inputs are finite; a program needn't handle non-finite values.
Results may differ from the reference program's by a relative error of at most 0.0034.
Values may be sent and summed in bfloat16 or wider, within the bound.
A program may use at most 128 MiB of HBM per device.

```python
import math
import jax
import jax.numpy as jnp
from jax import lax

D = 1024
PAIRS = 24576


def paired_draw(key):
    inner = jax.random.fold_in(key, 11)
    first_key, second_key, third_key = jax.random.split(inner, 3)
    query_vals = jnp.clip(jax.random.normal(first_key, (PAIRS, D), jnp.float32), -3.0, 3.0)
    passage_vals = jnp.clip(jax.random.normal(second_key, (PAIRS, D), jnp.float32), -3.0, 3.0)
    return (query_vals.astype(jnp.bfloat16), passage_vals.astype(jnp.bfloat16))


def draw_queries(key, part):
    return paired_draw(key)[0]


def draw_passages(key, part):
    return paired_draw(key)[1]


def place_ends(drawn, key, least, high):
    shape = drawn.shape
    place = [jax.random.randint(jax.random.fold_in(key, axis), (), 0, shape[axis]) for axis in range(len(shape))]
    drawn = drawn.at[tuple(place)].set(least)
    longest = shape.index(max(shape))
    place[longest] = (place[longest] + 1) % shape[longest]
    return drawn.at[tuple(place)].set(high)


def setup_inputs(seed: int = 0) -> dict:
    key_of = jax.random.split(jax.random.key(seed), 4)
    return {
        "queries": draw_queries(jax.random.fold_in(key_of[3], 71), 0),
        "passages": draw_passages(jax.random.fold_in(key_of[3], 71), 0),
        "positive": place_ends(jax.random.randint(key_of[2], (PAIRS,), 0, PAIRS), jax.random.fold_in(key_of[2], 1), 0, PAIRS - 1).astype(jnp.int32),
    }


def reference(queries, passages, positive):
    logit_scale = 3.0 / math.sqrt(D)
    block_rows = math.gcd(PAIRS, 512)
    block_count = PAIRS // block_rows
    query_blocks = queries.reshape(block_count, block_rows, D)
    target_blocks = positive.reshape(block_count, block_rows)
    column_ids = jnp.arange(PAIRS, dtype=jnp.int32)

    def one_block(carried, inputs):
        query_rows, targets = inputs
        scores = jnp.dot(query_rows, passages.T, preferred_element_type=jnp.float32) * logit_scale
        highest = lax.optimization_barrier(jnp.max(scores, axis=1))
        log_total = highest + jnp.log(lax.optimization_barrier(jnp.sum(jnp.exp(scores - highest[:, None]), axis=1)))
        onehot = (column_ids[None, :] == targets[:, None]).astype(jnp.float32)
        softmax_grad = (jnp.exp(scores - log_total[:, None]) - onehot).astype(jnp.bfloat16)
        query_grad = jnp.dot(softmax_grad, passages, preferred_element_type=jnp.float32).astype(jnp.bfloat16)
        carried = carried + jnp.dot(softmax_grad.T, query_rows, preferred_element_type=jnp.float32)
        return (carried, query_grad)
    start_grad = jnp.zeros((PAIRS, D), jnp.float32)
    passage_total, query_grads = lax.scan(one_block, start_grad, (query_blocks, target_blocks))
    return (query_grads.reshape(PAIRS, D), passage_total.astype(jnp.bfloat16))
```

```python
import functools
import math

import jax
import jax.numpy as jnp
from jax import lax
from jax.experimental import pallas as pl
from jax.experimental.pallas import tpu as pltpu
from jax.sharding import Mesh
from jax.sharding import PartitionSpec as P

BF16, F32 = jnp.bfloat16, jnp.float32
D = 1024
SCALE = 3.0 / math.sqrt(D)
QUARTER, HALF = 192, 384
BLOCK = 1536
GROUP = 768
COPIES = 208
NT = (((1,), (1,)), ((), ()))
TN = (((0,), (0,)), ((), ()))


def place(dx=0, dy=0, dz=0, dc=0):
    z = lax.rem(lax.axis_index("zh") * 4 + lax.axis_index("zl") + dz + 8, 8)
    return {
        "zl": lax.rem(z, 4),
        "x": lax.rem(lax.axis_index("x") + dx + 4, 4),
        "c": lax.rem(lax.axis_index("c") + dc, 2),
        "zh": lax.div(z, 4),
        "y": lax.rem(lax.axis_index("y") + dy + 4, 4),
    }


def kernel(
    q, p, pos, oq, op,
    qb, pb, posb, sc, sg, st,
    da, db, own_a, own_b, ra, rb, s2a, s2b, r2a, r2b, zs, zr,
    dps, dpr, sf, rf, sy, ry,
    ssem, rsem,
):
    x, y, c, zl, zh = (lax.axis_index(a) for a in ("x", "y", "c", "zl", "zh"))
    oc = 1 - c
    oz = 1 - zh
    sent = []

    def send(src, dst, **where):
        k = len(sent)
        copy = pltpu.make_async_remote_copy(
            src_ref=src, dst_ref=dst, send_sem=ssem.at[k], recv_sem=rsem.at[k],
            device_id=place(**where), device_id_type=pl.DeviceIdType.MESH,
        )
        copy.start()
        sent.append(copy)
        return copy

    def half_of(dz):
        return lax.div(lax.rem(zh * 4 + zl + dz, 8), 4)

    plane = [(dx, dy) for dx in range(4) for dy in range(4) if dx or dy]
    peers = [dict(dx=dx, dy=dy) for dx, dy in plane]
    peers += [dict(dz=1), dict(dz=-1), dict(dz=4), dict(dc=1)]
    barrier = pltpu.get_barrier_semaphore()
    for where in peers:
        pl.semaphore_signal(barrier, inc=1, device_id=place(**where), device_id_type=pl.DeviceIdType.MESH)
    pl.semaphore_wait(barrier, len(peers))

    swap = send(q.at[pl.ds(oz * 2, 2)], qb.at[0, zh, :, pl.ds(0, QUARTER)], dz=4)
    mine = pl.ds(pl.multiple_of(c * QUARTER, 16), QUARTER)
    spread = {}
    for d in (1, 3, 2):
        rows = pl.ds(pl.multiple_of(lax.rem(y + d, 4) * QUARTER, 16), QUARTER)
        spread[-d % 4] = send(p.at[rows], pb.at[-d % 4, zh, mine], dy=d)
    own_rows = pl.ds(pl.multiple_of(zh * HALF, 16), HALF)
    from_y, from_x = {}, {}

    def share(src, h, tag):
        for d in (1, 3, 2):
            from_y[-d % 4, tag] = send(src, qb.at[-d % 4, h, :, pl.ds(0, QUARTER)], dy=d)
            from_x[-d % 4, tag] = send(src, qb.at[0, h, :, pl.ds((-d % 4) * QUARTER, QUARTER)], dx=d)

    share(q.at[pl.ds(zh * 2, 2)], zh, 0)
    from_pos = {d: send(pos.at[zh], posb.at[-d % 4], dx=d) for d in (1, 3, 2)}
    for g in (0, 1):
        qb[0, zh, g, 0:QUARTER, :] = q[zh * 2 + g]
    posb[0] = pos[zh]
    pb[0, zh, mine, :] = p[pl.ds(pl.multiple_of(y * QUARTER, 16), QUARTER), :]

    def piece(dz, sub):
        rows = pl.ds(pl.multiple_of((dz % 4) * 2 * QUARTER + c * QUARTER, 16), QUARTER)
        ys = pl.ds(0, 4) if sub is None else pl.ds(sub * 2, 2)
        return ys, half_of(dz), rows

    ring, cores = {}, {}

    def pass_on(dz, sub, step):
        ys, h, rows = piece(dz, sub)
        to = (dz - step) % 8
        dst_rows = pl.ds(pl.multiple_of((to % 4) * 2 * QUARTER + c * QUARTER, 16), QUARTER)
        ring[to, sub] = send(pb.at[ys, h, rows], pb.at[ys, h, dst_rows], dz=step)

    def to_core(dz):
        ys, h, rows = piece(dz, None)
        cores[dz] = send(pb.at[ys, h, rows], pb.at[ys, h, rows], dc=1)

    spread[1].wait_recv()
    pass_on(0, 0, 1)
    pass_on(0, 0, -1)
    spread[3].wait_recv()
    spread[2].wait_recv()
    pass_on(0, 1, 1)
    pass_on(0, 1, -1)
    to_core(0)
    swap.wait_recv()
    share(qb.at[0, oz, :, pl.ds(0, QUARTER)], oz, 1)

    def hop(n):
        for sub in (0, 1):
            for dz, step in ((n, -1), (8 - n, 1)):
                ring[dz, sub].wait_recv()
                if n < 3 or (sub == 0) == (step == -1):
                    pass_on(dz, sub, step)
        to_core(n)
        to_core(8 - n)

    hop(1)
    second = []
    for k in (1, 3, 2):
        for tag in (0, 1):
            from_y[k, tag].wait_recv()
        for d in (1, 3, 2):
            ref = qb.at[k, :, 0, pl.ds(0, QUARTER)]
            second.append(send(ref, qb.at[k, :, 0, pl.ds((-d % 4) * QUARTER, QUARTER)], dx=d))
        for tag in (0, 1):
            from_x[k, tag].wait_recv()
        for d in (1, 3, 2):
            ref = qb.at[0, :, 1, pl.ds(k * QUARTER, QUARTER)]
            second.append(send(ref, qb.at[-d % 4, :, 1, pl.ds(k * QUARTER, QUARTER)], dy=d))
    hop(2)
    hop(3)
    for sub in (0, 1):
        ring[4, sub].wait_recv()
    to_core(4)
    for copy in second:
        copy.wait_recv()
    for copy in from_pos.values():
        copy.wait_recv()
    for dz in range(8):
        cores[dz].wait_recv()

    def wide(ref, *at):
        return jnp.concatenate([ref[(k, h, *at)] for k in range(4) for h in range(2)], axis=1)

    stats = {}
    for g in (0, 1):

        def scores(j, carry, g=g):
            top, total = carry
            rows = pl.ds(pl.multiple_of(j * HALF, 16), HALF)
            s = lax.dot_general(wide(pb, rows), wide(qb, g), NT, preferred_element_type=F32) * SCALE
            sc[g, rows, :] = s
            higher = jnp.maximum(top, jnp.max(s, axis=0, keepdims=True))
            total = total * jnp.exp(top - higher) + jnp.sum(jnp.exp(s - higher), axis=0, keepdims=True)
            return higher, total

        start = (jnp.full((1, GROUP), -3e38, F32), jnp.zeros((1, GROUP), F32))
        top, total = lax.fori_loop(0, 4, scores, start)
        for i in range(4):
            st[g, 0, i, 0:1, :] = top[:, i * QUARTER : (i + 1) * QUARTER]
            st[g, 0, i, 1:2, :] = total[:, i * QUARTER : (i + 1) * QUARTER]
        for dx, dy in plane:
            stats[g, dx, dy] = send(st.at[g, 0], st.at[g, (-dx % 4) * 4 + (-dy % 4)], dx=dx, dy=dy)

    stage_a, stage_b = {}, {}
    for g in (0, 1):
        for dx, dy in plane:
            stats[g, dx, dy].wait_recv()
        logs = []
        for i in range(4):
            pairs = [(k, (i - k // 4) % 4) for k in range(16)]
            tops = [st[g, k, n, 0:1, :] for k, n in pairs]
            high = functools.reduce(jnp.maximum, tops)
            total = sum(st[g, k, n, 1:2, :] * jnp.exp(t - high) for (k, n), t in zip(pairs, tops))
            logs.append(high + jnp.log(total))
        log_total = jnp.concatenate(logs, axis=1)
        targets = jnp.concatenate([posb[i, g] for i in range(4)], axis=1)

        def normal(j, carry, g=g, log_total=log_total, targets=targets):
            rows = pl.ds(pl.multiple_of(j * QUARTER, 16), QUARTER)
            owner = (lax.rem(zl + lax.div(j, 2), 4) * 4 + x) * 2 + lax.rem(j, 2)
            ids = lax.broadcasted_iota(jnp.int32, (QUARTER, GROUP), 0) + (owner * 768 + y * QUARTER)
            e = jnp.exp(sc[g, rows, :] - log_total)
            sg[g, rows, :] = jnp.where(ids == targets, e - 1.0, e).astype(BF16)
            return carry

        lax.fori_loop(0, 8, normal, 0)
        for k in (1, 3, 2, 0):
            rhs = jnp.concatenate([pb[k, 0], pb[k, 1]], axis=1)
            r = lax.dot_general(sg[g], rhs, TN, preferred_element_type=F32)
            if g == 0:
                own_a[k] = r[:QUARTER]
                for i in (1, 3, 2):
                    da[i, k] = r[i * QUARTER : (i + 1) * QUARTER].astype(BF16)
                    stage_a[-i % 4, k] = send(da.at[i, k], ra.at[-i % 4, k], dx=i)
            elif k:
                db[k] = r.astype(BF16)
                stage_b[-k % 4] = send(db.at[k], rb.at[-k % 4], dy=k)
            else:
                own_b[...] = r

    halves = {}

    def passages(s):
        def columns(k, carry):
            rows = slice(s * HALF, (s + 1) * HALF)
            r = sum(
                jnp.dot(
                    sg[g, rows, :],
                    jnp.concatenate([qb[k, h, g] for h in range(2)], axis=1),
                    preferred_element_type=F32,
                )
                for g in (0, 1)
            )
            for i in range(2):
                for h in range(2):
                    dps[s, i, h, k] = r[i * QUARTER : (i + 1) * QUARTER, h * 128 : (h + 1) * 128]
            return carry

        lax.fori_loop(0, 4, columns, 0)
        halves[s] = send(dps.at[s, oc], dpr.at[s], dc=1)

    def both(dz, k):
        h = half_of(dz)
        return dps[dz % 4, c, h, k] + dpr[dz % 4, h, k]

    sums = {}

    def add_on(way, n, sub, arrived):
        dz = (4 - n) if way == 0 else (4 + n)
        for i in range(2):
            v = both(dz, sub * 2 + i)
            if arrived:
                v = v + rf[way, n, sub, i].astype(F32)
            sf[way, n, sub, i] = v.astype(BF16)
        sums[way, n + 1, sub] = send(sf.at[way, n, sub], rf.at[way, n + 1, sub], dz=1 - 2 * way)

    passages(0)
    passages(3)
    halves[0].wait_recv()
    add_on(0, 0, 0, False)
    add_on(1, 0, 1, False)
    passages(1)
    halves[3].wait_recv()
    add_on(0, 1, 1, False)
    passages(2)
    halves[1].wait_recv()
    add_on(1, 1, 0, False)
    sums[0, 1, 0].wait_recv()
    add_on(0, 1, 0, True)
    sums[1, 1, 1].wait_recv()
    add_on(1, 1, 1, True)
    halves[2].wait_recv()

    def step(n):
        for way, sub in ((0, 1), (1, 0), (0, 0), (1, 1)):
            sums[way, n, sub].wait_recv()
            add_on(way, n, sub, True)

    step(2)

    final_a, final_b = {}, {}
    for k in (1, 3, 2, 0):
        for i in (1, 2, 3):
            stage_a[i, k].wait_recv()
        v = own_a[k] + sum(ra[i, k].astype(F32) for i in (1, 2, 3))
        if k:
            s2a[k] = v.astype(BF16)
            final_a[-k % 4] = send(s2a.at[k], r2a.at[-k % 4], dy=k)
        else:
            own_a[0] = v
    step(3)
    for i in (1, 2, 3):
        stage_b[i].wait_recv()
    for k in (1, 3, 2, 0):
        rows = slice(k * QUARTER, (k + 1) * QUARTER)
        v = own_b[rows, :] + sum(rb[i, rows, :].astype(F32) for i in (1, 2, 3))
        if k:
            s2b[k] = v.astype(BF16)
            final_b[-k % 4] = send(s2b.at[k], r2b.at[-k % 4], dx=k)
        else:
            own_b[rows, :] = v
    for k in (1, 2, 3):
        final_a[k].wait_recv()
        final_b[k].wait_recv()
    fa = own_a[0] + sum(r2a[k].astype(F32) for k in (1, 2, 3))
    fb = own_b[0:QUARTER, :] + sum(r2b[k].astype(F32) for k in (1, 2, 3))
    for h in range(2):
        zs[h, 0:QUARTER, :] = fa[:, h * 128 : (h + 1) * 128].astype(BF16)
        zs[h, QUARTER:HALF, :] = fb[:, h * 128 : (h + 1) * 128].astype(BF16)
    last = send(zs.at[oz], zr, dz=4)
    oq[own_rows, :] = zs[zh]

    for way, sub in ((0, 1), (1, 0), (0, 0), (1, 1)):
        sums[way, 4, sub].wait_recv()
    widths = {}
    for k in (1, 3, 2, 0):
        v = both(0, k) + rf[0, 4, k // 2, k % 2].astype(F32) + rf[1, 4, k // 2, k % 2].astype(F32)
        if k:
            sy[k] = v.astype(BF16)
            widths[-k % 4] = send(sy.at[k], ry.at[-k % 4], dy=k)
        else:
            op[pl.ds(pl.multiple_of(y * QUARTER, 16), QUARTER), :] = v.astype(BF16)
    for k in (1, 2, 3):
        widths[k].wait_recv()
        op[pl.ds(pl.multiple_of(lax.rem(y + k, 4) * QUARTER, 16), QUARTER), :] = ry[k]
    last.wait_recv()
    oq[pl.ds(pl.multiple_of(oz * HALF, 16), HALF), :] = zr[...]
    for copy in sent:
        copy.wait_send()


def local(queries, passages, positive):
    vmem = pl.BlockSpec(memory_space=pltpu.VMEM)
    shapes = [
        ((4, 2, 2, GROUP, 128), BF16),
        ((4, 2, BLOCK, 128), BF16),
        ((4, 2, 1, QUARTER), jnp.int32),
        ((2, BLOCK, GROUP), F32),
        ((2, BLOCK, GROUP), BF16),
        ((2, 16, 4, 2, QUARTER), F32),
        ((4, 4, QUARTER, 256), BF16),
        ((4, GROUP, 256), BF16),
        ((4, QUARTER, 256), F32),
        ((GROUP, 256), F32),
        ((4, 4, QUARTER, 256), BF16),
        ((4, GROUP, 256), BF16),
        ((4, QUARTER, 256), BF16),
        ((4, QUARTER, 256), BF16),
        ((4, QUARTER, 256), BF16),
        ((4, QUARTER, 256), BF16),
        ((2, HALF, 128), BF16),
        ((HALF, 128), BF16),
        ((4, 2, 2, 4, QUARTER, 128), F32),
        ((4, 2, 4, QUARTER, 128), F32),
        ((2, 4, 2, 2, QUARTER, 128), BF16),
        ((2, 5, 2, 2, QUARTER, 128), BF16),
        ((4, QUARTER, 128), BF16),
        ((4, QUARTER, 128), BF16),
    ]
    return pl.pallas_call(
        kernel,
        out_shape=(jax.ShapeDtypeStruct((768, 128), BF16), jax.ShapeDtypeStruct((768, 128), BF16)),
        in_specs=[vmem, vmem, vmem],
        out_specs=(vmem, vmem),
        scratch_shapes=[pltpu.VMEM(s, t) for s, t in shapes]
        + [pltpu.SemaphoreType.DMA((COPIES,)), pltpu.SemaphoreType.DMA((COPIES,))],
        compiler_params=pltpu.CompilerParams(
            collective_id=0, has_side_effects=True, vmem_limit_bytes=62 * 2**20
        ),
    )(queries.reshape(4, QUARTER, 128), passages, positive.reshape(2, 2, 1, QUARTER))


def solution(mesh):
    finer = Mesh(mesh.devices.reshape(4, 4, 2, 2, 4), ("zl", "x", "c", "zh", "y"))
    dp, mp = ("zl", "x", "c"), ("zh", "y")
    return jax.shard_map(
        local,
        mesh=finer,
        in_specs=(P(dp, mp), P(dp, mp), P(dp)),
        out_specs=(P(dp, mp), P(dp, mp)),
        check_vma=False,
    )
```

```python
import functools
import math

import jax
import jax.numpy as jnp
from jax import lax
from jax.experimental import pallas as pl
from jax.experimental.pallas import tpu as pltpu
from jax.sharding import Mesh
from jax.sharding import PartitionSpec as P

BF16, F32 = jnp.bfloat16, jnp.float32
D = 1024
SCALE = 3.0 / math.sqrt(D)
EIGHTH, QUARTER, HALF = 96, 192, 384
BLOCK = 1536
GROUP = 768
ARRIVALS, DEPARTURES = 73, 25
NT = (((1,), (1,)), ((), ()))
TN = (((0,), (0,)), ((), ()))


def place(dx=0, dy=0, dz=0, dc=0):
    z = lax.rem(lax.axis_index("zh") * 4 + lax.axis_index("zl") + dz + 8, 8)
    return {
        "zl": lax.rem(z, 4),
        "x": lax.rem(lax.axis_index("x") + dx + 4, 4),
        "c": lax.rem(lax.axis_index("c") + dc, 2),
        "zh": lax.div(z, 4),
        "y": lax.rem(lax.axis_index("y") + dy + 4, 4),
    }


def kernel(
    q_hbm, p_hbm, pos_hbm, oq, op,
    q, p, pos, qb, pb, posb, sc, sg, st,
    da, db, own_a, own_b, ra, rb, s2a, s2b, r2a, r2b, zs, zr,
    dps, dpr, sf, rf, sy, ry,
    ssem, rsem, isem,
):
    x, y, c, zl, zh = (lax.axis_index(a) for a in ("x", "y", "c", "zl", "zh"))
    oc = 1 - c
    oz = 1 - zh
    arrivals, departures, leaving = {}, {}, {}

    def send(src, dst, tag, out=None, **where):
        out = tag if out is None else out
        copy = pltpu.make_async_remote_copy(
            src_ref=src, dst_ref=dst,
            send_sem=ssem.at[departures.setdefault(out, len(departures))],
            recv_sem=rsem.at[arrivals.setdefault(tag, len(arrivals))],
            device_id=place(**where), device_id_type=pl.DeviceIdType.MESH,
        )
        copy.start()
        leaving.setdefault(out, []).append(dst)

    def arrived(tag, ref):
        pltpu.make_async_copy(ref, ref, rsem.at[arrivals[tag]]).wait()

    def left(out, ref):
        pltpu.make_async_copy(ref, ref, ssem.at[departures[out]]).wait()

    def half_of(dz):
        return lax.div(lax.rem(zh * 4 + zl + dz, 8), 4)

    plane = [(dx, dy) for dx in range(4) for dy in range(4) if dx or dy]
    peers = [dict(dx=dx, dy=dy) for dx, dy in plane]
    peers += [dict(dz=1), dict(dz=-1), dict(dz=4), dict(dc=1)]
    inputs = [
        pltpu.make_async_copy(a, b, isem.at[k]) for k, (a, b) in enumerate(((q_hbm, q), (p_hbm, p), (pos_hbm, pos)))
    ]
    for copy in inputs:
        copy.start()
    barrier = pltpu.get_barrier_semaphore()
    for where in peers:
        pl.semaphore_signal(barrier, inc=1, device_id=place(**where), device_id_type=pl.DeviceIdType.MESH)
    pl.semaphore_wait(barrier, len(peers))

    for copy in inputs:
        copy.wait()

    mine = pl.ds(pl.multiple_of(c * QUARTER, 16), QUARTER)
    send(q.at[pl.ds(oz * 2, 2)], qb.at[0, zh, :, pl.ds(0, QUARTER)], "swap", dz=4)
    for d in (1, 3, 2):
        rows = pl.ds(pl.multiple_of(lax.rem(y + d, 4) * QUARTER, 16), QUARTER)
        send(p.at[rows], pb.at[-d % 4, zh, mine], ("spread", -d % 4), "spread", dy=d)

    def share(src, h, tag):
        for d in (1, 3, 2):
            send(src, qb.at[-d % 4, h, :, pl.ds(0, QUARTER)], ("y", -d % 4, tag), ("share", tag), dy=d)
            send(src, qb.at[0, h, :, pl.ds((-d % 4) * QUARTER, QUARTER)], ("x", -d % 4, tag), ("share", tag), dx=d)

    share(q.at[pl.ds(zh * 2, 2)], zh, 0)
    for d in (1, 3, 2):
        send(pos, posb.at[-d % 4], "pos", dx=d)
    for g in (0, 1):
        qb[0, zh, g, 0:QUARTER, :] = q[zh * 2 + g]
    posb[0] = pos[...]
    pb[0, zh, mine, :] = p[pl.ds(pl.multiple_of(y * QUARTER, 16), QUARTER), :]

    def piece(dz, sub):
        rows = pl.ds(pl.multiple_of((dz % 4) * 2 * QUARTER + c * QUARTER, 16), QUARTER)
        ys = pl.ds(0, 4) if sub is None else pl.ds(sub * 2, 2)
        return ys, half_of(dz), rows

    def pass_on(dz, sub, step):
        ys, h, rows = piece(dz, sub)
        to = (dz - step) % 8
        to_rows = pl.ds(pl.multiple_of((to % 4) * 2 * QUARTER + c * QUARTER, 16), QUARTER)
        send(pb.at[ys, h, rows], pb.at[ys, h, to_rows], ("ring", to, sub), "ring", dz=step)

    def ring_arrived(dz, sub):
        arrived(("ring", dz, sub), pb.at[pl.ds(0, 2), 0, pl.ds(0, QUARTER)])

    def to_core(dz):
        ys, h, rows = piece(dz, None)
        send(pb.at[ys, h, rows], pb.at[ys, h, rows], ("core", dz), "core", dc=1)

    def core_arrived(*dzs):
        for dz in dzs:
            arrived(("core", dz), pb.at[:, 0, pl.ds(0, QUARTER)])

    def spread_arrived(*ds):
        for d in ds:
            arrived(("spread", d), pb.at[0, 0, pl.ds(0, QUARTER)])

    def groups_of(groups):
        return pl.ds(0, 2) if groups == "both" else pl.ds(groups, 1)

    def spread_y(k, tag, h, groups):
        gs, rows = groups_of(groups), pl.ds(0, EIGHTH)
        for d in (1, 3, 2):
            to_rows = pl.ds((-d % 4) * QUARTER, EIGHTH)
            send(qb.at[k, h, gs, rows], qb.at[k, h, gs, to_rows], ("second", tag, groups), dx=d)

    def spread_x(k, tag, h, groups):
        gs, rows = groups_of(groups), pl.ds(k * QUARTER + EIGHTH, EIGHTH)
        for d in (1, 3, 2):
            send(qb.at[0, h, gs, rows], qb.at[-d % 4, h, gs, rows], ("second", tag, groups), dy=d)

    def share_arrived(way, k, tag):
        arrived((way, k, tag), qb.at[0, 0, :, pl.ds(0, QUARTER)])

    def second_arrived(tag, groups):
        arrived(("second", tag, groups), qb.at[pl.ds(0, 3), 0, groups_of(groups), pl.ds(0, 576)])

    def hop(n):
        for sub in (0, 1):
            for dz, step in ((n, -1), (8 - n, 1)):
                ring_arrived(dz, sub)
                if n < 3 or (sub == 0) == (step == -1):
                    pass_on(dz, sub, step)
        to_core(n)
        to_core(8 - n)

    spread_arrived(1)
    pass_on(0, 0, 1)
    pass_on(0, 0, -1)
    spread_arrived(3, 2)
    pass_on(0, 1, 1)
    pass_on(0, 1, -1)
    to_core(0)
    share_arrived("x", 1, 0)
    spread_x(1, 0, zh, "both")
    share_arrived("y", 1, 0)
    spread_y(1, 0, zh, "both")
    arrived("swap", qb.at[0, 0, :, pl.ds(0, QUARTER)])
    share(qb.at[0, oz, :, pl.ds(0, QUARTER)], oz, 1)
    for k in (3, 2):
        share_arrived("x", k, 0)
        spread_x(k, 0, zh, "both")
        share_arrived("y", k, 0)
        spread_y(k, 0, zh, "both")
    hop(1)
    hop(2)
    for k in (1, 3, 2):
        share_arrived("x", k, 1)
        share_arrived("y", k, 1)
    for g in (0, 1):
        for k in (1, 3, 2):
            spread_x(k, 1, oz, g)
            spread_y(k, 1, oz, g)
    hop(3)
    arrived("pos", posb.at[pl.ds(1, 3)])
    second_arrived(0, "both")
    second_arrived(1, 0)

    def wide(ref, *at):
        return jnp.concatenate([ref[(k, h, *at)] for k in range(4) for h in range(2)], axis=1)

    best = {0: None, 1: None}

    def scores(g, n):
        rows = slice(n * HALF, (n + 1) * HALF)
        sc[g, rows, :] = lax.dot_general(wide(pb, rows), wide(qb, g), NT, preferred_element_type=F32) * SCALE

    def tally(g, n):
        s = sc[g, n * HALF : (n + 1) * HALF, :]
        high = jnp.max(s, axis=0, keepdims=True)
        if best[g] is None:
            best[g] = high, jnp.sum(jnp.exp(s - high), axis=0, keepdims=True)
        else:
            top, total = best[g]
            higher = jnp.maximum(top, high)
            total = total * jnp.exp(top - higher) + jnp.sum(jnp.exp(s - higher), axis=0, keepdims=True)
            best[g] = higher, total

    def publish(g):
        top, total = best[g]
        for i in range(4):
            st[g, 0, i, 0:1, :] = top[:, i * QUARTER : (i + 1) * QUARTER]
            st[g, 0, i, 1:2, :] = total[:, i * QUARTER : (i + 1) * QUARTER]
        for dx, dy in plane:
            send(st.at[g, 0], st.at[g, (-dx % 4) * 4 + (-dy % 4)], ("stats", g), dx=dx, dy=dy)

    core_arrived(2, 6)
    scores(0, 2)
    core_arrived(1, 5, 3, 7)
    scores(0, 1)
    tally(0, 2)
    scores(0, 3)
    tally(0, 1)
    for sub in (0, 1):
        ring_arrived(4, sub)
    to_core(4)
    second_arrived(1, 1)
    scores(1, 2)
    tally(0, 3)
    core_arrived(0, 4)
    scores(0, 0)
    tally(1, 2)
    scores(1, 1)
    tally(0, 0)
    publish(0)
    scores(1, 3)
    tally(1, 1)
    scores(1, 0)
    tally(1, 3)
    tally(1, 0)
    publish(1)

    def normalise(g):
        arrived(("stats", g), st.at[g, pl.ds(1, 15)])
        logs = []
        for i in range(4):
            pairs = [(k, (i - k // 4) % 4) for k in range(16)]
            tops = [st[g, k, n, 0:1, :] for k, n in pairs]
            high = functools.reduce(jnp.maximum, tops)
            total = sum(st[g, k, n, 1:2, :] * jnp.exp(t - high) for (k, n), t in zip(pairs, tops))
            logs.append(high + jnp.log(total))
        log_total = jnp.concatenate(logs, axis=1)
        targets = []
        for i in range(4):
            three = jnp.concatenate([posb[i, pl.ds(zh * 3 + t, 1), :] for t in range(3)], axis=1)
            targets.append(three[:, g * QUARTER : (g + 1) * QUARTER])
        targets = jnp.concatenate(targets, axis=1)

        def normal(j, carry, g=g, log_total=log_total, targets=targets):
            rows = pl.ds(pl.multiple_of(j * QUARTER, 16), QUARTER)
            owner = (lax.rem(zl + lax.div(j, 2), 4) * 4 + x) * 2 + lax.rem(j, 2)
            ids = lax.broadcasted_iota(jnp.int32, (QUARTER, GROUP), 0) + (owner * 768 + y * QUARTER)
            e = jnp.exp(sc[g, rows, :] - log_total)
            sg[g, rows, :] = jnp.where(ids == targets, e - 1.0, e).astype(BF16)
            return carry

        lax.fori_loop(0, 8, normal, 0)

    def query_gradients(g):
        r = lax.dot_general(sg[g], wide(pb), TN, preferred_element_type=F32)
        for i in (1, 3, 2, 0):
            for k in range(4):
                rows, columns = slice(i * QUARTER, i * QUARTER + EIGHTH), slice(k * 256, (k + 1) * 256)
                if i:
                    da[g, i, k] = r[rows, columns].astype(BF16)
                else:
                    own_a[g, k] = r[rows, columns]
            if i:
                send(da.at[g, i], ra.at[g, -i % 4], ("a", g), dx=i)
        for k in (1, 3, 2, 0):
            for i in range(4):
                rows, columns = slice(i * QUARTER + EIGHTH, (i + 1) * QUARTER), slice(k * 256, (k + 1) * 256)
                if k:
                    db[g, k, i] = r[rows, columns].astype(BF16)
                else:
                    own_b[g, i] = r[rows, columns]
            if k:
                send(db.at[g, k], rb.at[g, -k % 4], ("b", g), dy=k)

    def passages(s):
        rows = slice(s * HALF, (s + 1) * HALF)
        r = jnp.dot(
            jnp.concatenate([sg[g, rows, :] for g in range(2)], axis=1),
            jnp.concatenate([wide(qb, g) for g in range(2)], axis=0),
            preferred_element_type=F32,
        )
        for k in range(4):
            for i in range(2):
                for h in range(2):
                    column = k * 256 + h * 128
                    dps[s, i, h, k] = r[i * QUARTER : (i + 1) * QUARTER, column : column + 128]
        send(dps.at[s, oc], dpr.at[s], ("half", s), "half", dc=1)

    def half_arrived(*ss):
        for s in ss:
            arrived(("half", s), dpr.at[s])

    def both(dz, k):
        h = half_of(dz)
        return dps[dz % 4, c, h, k] + dpr[dz % 4, h, k]

    def add_on(way, n, sub, first=False):
        dz = (4 - n) if way == 0 else (4 + n)
        for i in range(2):
            v = both(dz, sub * 2 + i)
            if not first:
                v = v + rf[way, n, sub, i].astype(F32)
            sf[way, n, sub, i] = v.astype(BF16)
        send(sf.at[way, n, sub], rf.at[way, n + 1, sub], ("sum", way, n + 1, sub), "sum", dz=1 - 2 * way)

    def sum_arrived(way, n, sub):
        arrived(("sum", way, n, sub), rf.at[way, n, sub])

    def step(n):
        for way, sub in ((0, 1), (1, 0), (0, 0), (1, 1)):
            sum_arrived(way, n, sub)
            add_on(way, n, sub)

    def second_stage(g):
        arrived(("a", g), ra.at[g, pl.ds(1, 3)])
        arrived(("b", g), rb.at[g, pl.ds(1, 3)])
        for k in (1, 3, 2, 0):
            va = own_a[g, k] + sum(ra[g, i, k].astype(F32) for i in (1, 2, 3))
            vb = own_b[g, k] + sum(rb[g, i, k].astype(F32) for i in (1, 2, 3))
            if k:
                s2a[g, k] = va.astype(BF16)
                send(s2a.at[g, k], r2a.at[g, -k % 4], ("a2", g), dy=k)
                s2b[g, k] = vb.astype(BF16)
                send(s2b.at[g, k], r2b.at[g, -k % 4], ("b2", g), dx=k)
            else:
                own_a[g, 0] = va
                own_b[g, 0] = vb

    def third_stage(g):
        arrived(("a2", g), r2a.at[g, pl.ds(1, 3)])
        arrived(("b2", g), r2b.at[g, pl.ds(1, 3)])
        fa = own_a[g, 0] + sum(r2a[g, k].astype(F32) for k in (1, 2, 3))
        fb = own_b[g, 0] + sum(r2b[g, k].astype(F32) for k in (1, 2, 3))
        for h in range(2):
            zs[h, g, 0:EIGHTH, :] = fa[:, h * 128 : (h + 1) * 128].astype(BF16)
            zs[h, g, EIGHTH:QUARTER, :] = fb[:, h * 128 : (h + 1) * 128].astype(BF16)
        send(zs.at[oz, g], zr.at[g], ("last", g), dz=4)
        oq[pl.ds(pl.multiple_of(zh * HALF + g * QUARTER, 16), QUARTER), :] = zs[zh, g]

    normalise(0)
    query_gradients(0)
    normalise(1)
    passages(0)
    passages(3)
    half_arrived(0)
    add_on(0, 0, 0, True)
    add_on(1, 0, 1, True)
    passages(1)
    half_arrived(3)
    add_on(0, 1, 1, True)
    passages(2)
    half_arrived(1)
    add_on(1, 1, 0, True)
    query_gradients(1)
    for way, sub in ((0, 0), (1, 1)):
        sum_arrived(way, 1, sub)
        add_on(way, 1, sub)
    half_arrived(2)
    second_stage(0)
    step(2)
    second_stage(1)
    third_stage(0)
    step(3)
    third_stage(1)

    for way, sub in ((0, 1), (1, 0), (0, 0), (1, 1)):
        sum_arrived(way, 4, sub)
    for k in (1, 3, 2, 0):
        v = both(0, k) + rf[0, 4, k // 2, k % 2].astype(F32) + rf[1, 4, k // 2, k % 2].astype(F32)
        if k:
            sy[k] = v.astype(BF16)
            send(sy.at[k], ry.at[-k % 4], "widths", dy=k)
        else:
            op[pl.ds(pl.multiple_of(y * QUARTER, 16), QUARTER), :] = v.astype(BF16)
    arrived("widths", ry.at[pl.ds(1, 3)])
    for k in (1, 2, 3):
        op[pl.ds(pl.multiple_of(lax.rem(y + k, 4) * QUARTER, 16), QUARTER), :] = ry[k]
    for g in (0, 1):
        arrived(("last", g), zr.at[g])
        oq[pl.ds(pl.multiple_of(oz * HALF + g * QUARTER, 16), QUARTER), :] = zr[g]
    rest = {
        "spread": pb.at[pl.ds(0, 3), 0, pl.ds(0, QUARTER)],
        "ring": pb.at[:, 0, pl.ds(0, 1344)],
        "core": pb.at[:, 0],
        ("share", 0): qb.at[pl.ds(0, 3), 0, 0],
        ("share", 1): qb.at[pl.ds(0, 3), 0, 0],
        "pos": posb.at[pl.ds(1, 3)],
        ("second", 0, "both"): qb.at[pl.ds(0, 3), 0, :, pl.ds(0, 576)],
        ("second", 1, 0): qb.at[pl.ds(0, 3), 0, pl.ds(0, 1), pl.ds(0, 576)],
        ("second", 1, 1): qb.at[pl.ds(0, 3), 0, pl.ds(0, 1), pl.ds(0, 576)],
        "half": dpr,
        "sum": pb.at[:, 0, pl.ds(0, 1344)],
        "widths": ry.at[pl.ds(1, 3)],
    }
    for g in (0, 1):
        rest["stats", g] = st.at[g, pl.ds(1, 15)]
        rest["a", g], rest["b", g] = ra.at[g, pl.ds(1, 3)], rb.at[g, pl.ds(1, 3)]
        rest["a2", g], rest["b2", g] = r2a.at[g, pl.ds(1, 3)], r2b.at[g, pl.ds(1, 3)]
    for out, dsts in leaving.items():
        ref = dsts[0] if len(dsts) == 1 else rest[out]
        size = lambda r: math.prod(r.shape) * r.dtype.itemsize
        assert size(ref) == sum(size(d) for d in dsts), out
        left(out, ref)
    assert (len(arrivals), len(departures)) == (ARRIVALS, DEPARTURES), (len(arrivals), len(departures))


def local(queries, passages, positive):
    vmem = pl.BlockSpec(memory_space=pltpu.VMEM)
    shapes = [
        ((4, QUARTER, 128), BF16),
        ((768, 128), BF16),
        ((6, 128), jnp.int32),
        ((4, 2, 2, GROUP, 128), BF16),
        ((4, 2, BLOCK, 128), BF16),
        ((4, 6, 128), jnp.int32),
        ((2, BLOCK, GROUP), F32),
        ((2, BLOCK, GROUP), BF16),
        ((2, 16, 4, 2, QUARTER), F32),
        ((2, 4, 4, EIGHTH, 256), BF16),
        ((2, 4, 4, EIGHTH, 256), BF16),
        ((2, 4, EIGHTH, 256), F32),
        ((2, 4, EIGHTH, 256), F32),
        ((2, 4, 4, EIGHTH, 256), BF16),
        ((2, 4, 4, EIGHTH, 256), BF16),
        ((2, 4, EIGHTH, 256), BF16),
        ((2, 4, EIGHTH, 256), BF16),
        ((2, 4, EIGHTH, 256), BF16),
        ((2, 4, EIGHTH, 256), BF16),
        ((2, 2, QUARTER, 128), BF16),
        ((2, QUARTER, 128), BF16),
        ((4, 2, 2, 4, QUARTER, 128), F32),
        ((4, 2, 4, QUARTER, 128), F32),
        ((2, 4, 2, 2, QUARTER, 128), BF16),
        ((2, 5, 2, 2, QUARTER, 128), BF16),
        ((4, QUARTER, 128), BF16),
        ((4, QUARTER, 128), BF16),
    ]
    return pl.pallas_call(
        kernel,
        out_shape=(pltpu.VMEM((768, 128), BF16), pltpu.VMEM((768, 128), BF16)),
        in_specs=[pl.BlockSpec(memory_space=pl.ANY)] * 3,
        out_specs=(vmem, vmem),
        scratch_shapes=[pltpu.VMEM(s, t) for s, t in shapes]
        + [pltpu.SemaphoreType.DMA((n,)) for n in (DEPARTURES, ARRIVALS, 3)],
        compiler_params=pltpu.CompilerParams(
            collective_id=0, has_side_effects=True, vmem_limit_bytes=62 * 2**20
        ),
    )(queries.reshape(4, QUARTER, 128), passages, positive.reshape(6, 128))


def solution(mesh):
    finer = Mesh(mesh.devices.reshape(4, 4, 2, 2, 4), ("zl", "x", "c", "zh", "y"))
    dp, mp = ("zl", "x", "c"), ("zh", "y")
    return jax.shard_map(
        local,
        mesh=finer,
        in_specs=(P(dp, mp), P(dp, mp), P(dp)),
        out_specs=(P(dp, mp), P(dp, mp)),
        check_vma=False,
    )
```

```python
import functools
import math

import jax
import jax.numpy as jnp
from jax import lax
from jax.experimental import pallas as pl
from jax.experimental.pallas import tpu as pltpu
from jax.sharding import Mesh
from jax.sharding import PartitionSpec as P

BF16, F32 = jnp.bfloat16, jnp.float32
D = 1024
SCALE = 3.0 / math.sqrt(D)
EIGHTH, QUARTER, HALF = 96, 192, 384
BLOCK = 1536
GROUP = 768
ARRIVALS, DEPARTURES = 73, 25
NT = (((1,), (1,)), ((), ()))
TN = (((0,), (0,)), ((), ()))


def place(dx=0, dy=0, dz=0, dc=0):
    z = lax.rem(lax.axis_index("zh") * 4 + lax.axis_index("zl") + dz + 8, 8)
    return {
        "zl": lax.rem(z, 4),
        "x": lax.rem(lax.axis_index("x") + dx + 4, 4),
        "c": lax.rem(lax.axis_index("c") + dc, 2),
        "zh": lax.div(z, 4),
        "y": lax.rem(lax.axis_index("y") + dy + 4, 4),
    }


def kernel(
    q_hbm, p_hbm, pos_hbm, oq, op,
    q, p, pos, qb, pb, posb, sc, sg, st,
    da, db, own_a, own_b, ra, rb, s2a, s2b, r2a, r2b, zs, zr,
    dps, dpr, sf, rf, sy, ry,
    ssem, rsem, isem,
):
    x, y, c, zl, zh = (lax.axis_index(a) for a in ("x", "y", "c", "zl", "zh"))
    oc = 1 - c
    oz = 1 - zh
    arrivals, departures, leaving = {}, {}, {}

    def send(src, dst, tag, out=None, **where):
        out = tag if out is None else out
        copy = pltpu.make_async_remote_copy(
            src_ref=src, dst_ref=dst,
            send_sem=ssem.at[departures.setdefault(out, len(departures))],
            recv_sem=rsem.at[arrivals.setdefault(tag, len(arrivals))],
            device_id=place(**where), device_id_type=pl.DeviceIdType.MESH,
        )
        copy.start()
        leaving.setdefault(out, []).append(dst)

    def arrived(tag, ref):
        pltpu.make_async_copy(ref, ref, rsem.at[arrivals[tag]]).wait()

    def left(out, ref):
        pltpu.make_async_copy(ref, ref, ssem.at[departures[out]]).wait()

    def half_of(dz):
        return lax.div(lax.rem(zh * 4 + zl + dz, 8), 4)

    plane = [(dx, dy) for dx in range(4) for dy in range(4) if dx or dy]
    peers = [dict(dx=dx, dy=dy) for dx, dy in plane]
    peers += [dict(dz=1), dict(dz=-1), dict(dz=4), dict(dc=1)]
    inputs = [
        pltpu.make_async_copy(a, b, isem.at[k]) for k, (a, b) in enumerate(((q_hbm, q), (p_hbm, p), (pos_hbm, pos)))
    ]
    for copy in inputs:
        copy.start()
    barrier = pltpu.get_barrier_semaphore()
    for where in peers:
        pl.semaphore_signal(barrier, inc=1, device_id=place(**where), device_id_type=pl.DeviceIdType.MESH)
    pl.semaphore_wait(barrier, len(peers))

    for copy in inputs:
        copy.wait()

    mine = pl.ds(pl.multiple_of(c * QUARTER, 16), QUARTER)
    send(q.at[pl.ds(oz * 2, 2)], qb.at[0, zh, :, pl.ds(0, QUARTER)], "swap", dz=4)
    for d in (1, 3, 2):
        rows = pl.ds(pl.multiple_of(lax.rem(y + d, 4) * QUARTER, 16), QUARTER)
        send(p.at[rows], pb.at[-d % 4, zh, mine], ("spread", -d % 4), "spread", dy=d)

    def share(src, h, tag):
        for d in (1, 3, 2):
            send(src, qb.at[-d % 4, h, :, pl.ds(0, QUARTER)], ("y", -d % 4, tag), ("share", tag), dy=d)
            send(src, qb.at[0, h, :, pl.ds((-d % 4) * QUARTER, QUARTER)], ("x", -d % 4, tag), ("share", tag), dx=d)

    share(q.at[pl.ds(zh * 2, 2)], zh, 0)
    for d in (1, 3, 2):
        send(pos, posb.at[-d % 4], "pos", dx=d)
    for g in (0, 1):
        qb[0, zh, g, 0:QUARTER, :] = q[zh * 2 + g]
    posb[0] = pos[...]
    pb[0, zh, mine, :] = p[pl.ds(pl.multiple_of(y * QUARTER, 16), QUARTER), :]

    def piece(dz, sub):
        rows = pl.ds(pl.multiple_of((dz % 4) * 2 * QUARTER + c * QUARTER, 16), QUARTER)
        ys = pl.ds(0, 4) if sub is None else pl.ds(sub * 2, 2)
        return ys, half_of(dz), rows

    def pass_on(dz, sub, step):
        ys, h, rows = piece(dz, sub)
        to = (dz - step) % 8
        to_rows = pl.ds(pl.multiple_of((to % 4) * 2 * QUARTER + c * QUARTER, 16), QUARTER)
        send(pb.at[ys, h, rows], pb.at[ys, h, to_rows], ("ring", to, sub), "ring", dz=step)

    def ring_arrived(dz, sub):
        arrived(("ring", dz, sub), pb.at[pl.ds(0, 2), 0, pl.ds(0, QUARTER)])

    def to_core(dz):
        ys, h, rows = piece(dz, None)
        send(pb.at[ys, h, rows], pb.at[ys, h, rows], ("core", dz), "core", dc=1)

    def core_arrived(*dzs):
        for dz in dzs:
            arrived(("core", dz), pb.at[:, 0, pl.ds(0, QUARTER)])

    def spread_arrived(*ds):
        for d in ds:
            arrived(("spread", d), pb.at[0, 0, pl.ds(0, QUARTER)])

    def groups_of(groups):
        return pl.ds(0, 2) if groups == "both" else pl.ds(groups, 1)

    def spread_y(k, tag, h, groups):
        gs, rows = groups_of(groups), pl.ds(0, EIGHTH)
        for d in (1, 3, 2):
            to_rows = pl.ds((-d % 4) * QUARTER, EIGHTH)
            send(qb.at[k, h, gs, rows], qb.at[k, h, gs, to_rows], ("second", tag, groups), dx=d)

    def spread_x(k, tag, h, groups):
        gs, rows = groups_of(groups), pl.ds(k * QUARTER + EIGHTH, EIGHTH)
        for d in (1, 3, 2):
            send(qb.at[0, h, gs, rows], qb.at[-d % 4, h, gs, rows], ("second", tag, groups), dy=d)

    def share_arrived(way, k, tag):
        arrived((way, k, tag), qb.at[0, 0, :, pl.ds(0, QUARTER)])

    def second_arrived(tag, groups):
        arrived(("second", tag, groups), qb.at[pl.ds(0, 3), 0, groups_of(groups), pl.ds(0, 576)])

    def hop(n):
        for sub in (0, 1):
            for dz, step in ((n, -1), (8 - n, 1)):
                ring_arrived(dz, sub)
                if n < 3 or (sub == 0) == (step == -1):
                    pass_on(dz, sub, step)
        to_core(n)
        to_core(8 - n)

    spread_arrived(1)
    pass_on(0, 0, 1)
    pass_on(0, 0, -1)
    spread_arrived(3, 2)
    pass_on(0, 1, 1)
    pass_on(0, 1, -1)
    to_core(0)
    share_arrived("x", 1, 0)
    spread_x(1, 0, zh, "both")
    share_arrived("y", 1, 0)
    spread_y(1, 0, zh, "both")
    arrived("swap", qb.at[0, 0, :, pl.ds(0, QUARTER)])
    share(qb.at[0, oz, :, pl.ds(0, QUARTER)], oz, 1)
    for k in (3, 2):
        share_arrived("x", k, 0)
        spread_x(k, 0, zh, "both")
        share_arrived("y", k, 0)
        spread_y(k, 0, zh, "both")
    hop(1)
    hop(2)
    for k in (1, 3, 2):
        share_arrived("x", k, 1)
        share_arrived("y", k, 1)
    for g in (0, 1):
        for k in (1, 3, 2):
            spread_x(k, 1, oz, g)
            spread_y(k, 1, oz, g)
    hop(3)
    arrived("pos", posb.at[pl.ds(1, 3)])
    second_arrived(0, "both")
    second_arrived(1, 0)

    def wide(ref, *at):
        return jnp.concatenate([ref[(k, h, *at)] for k in range(4) for h in range(2)], axis=1)

    best = {0: None, 1: None}

    def scores(g, n):
        rows = slice(n * HALF, (n + 1) * HALF)
        sc[g, rows, :] = lax.dot_general(wide(pb, rows), wide(qb, g), NT, preferred_element_type=F32) * SCALE

    def tally(g, n):
        s = sc[g, n * HALF : (n + 1) * HALF, :]
        high = jnp.max(s, axis=0, keepdims=True)
        if best[g] is None:
            best[g] = high, jnp.sum(jnp.exp(s - high), axis=0, keepdims=True)
        else:
            top, total = best[g]
            higher = jnp.maximum(top, high)
            total = total * jnp.exp(top - higher) + jnp.sum(jnp.exp(s - higher), axis=0, keepdims=True)
            best[g] = higher, total

    def publish(g):
        top, total = best[g]
        for i in range(4):
            st[g, 0, i, 0:1, :] = top[:, i * QUARTER : (i + 1) * QUARTER]
            st[g, 0, i, 1:2, :] = total[:, i * QUARTER : (i + 1) * QUARTER]
        for dx, dy in plane:
            send(st.at[g, 0], st.at[g, (-dx % 4) * 4 + (-dy % 4)], ("stats", g), dx=dx, dy=dy)

    core_arrived(2, 6)
    scores(0, 2)
    for sub in (0, 1):
        ring_arrived(4, sub)
    to_core(4)
    core_arrived(1, 5, 3, 7)
    scores(0, 1)
    tally(0, 2)
    scores(0, 3)
    tally(0, 1)
    second_arrived(1, 1)
    scores(1, 2)
    tally(0, 3)
    core_arrived(0, 4)
    scores(0, 0)
    tally(1, 2)
    tally(0, 0)
    publish(0)
    scores(1, 1)
    scores(1, 3)
    tally(1, 1)
    scores(1, 0)
    tally(1, 3)
    tally(1, 0)
    publish(1)

    logs_of, targets_of = {}, {}

    def normaliser(g):
        arrived(("stats", g), st.at[g, pl.ds(1, 15)])
        logs = []
        for i in range(4):
            pairs = [(k, (i - k // 4) % 4) for k in range(16)]
            tops = [st[g, k, n, 0:1, :] for k, n in pairs]
            high = functools.reduce(jnp.maximum, tops)
            total = sum(st[g, k, n, 1:2, :] * jnp.exp(t - high) for (k, n), t in zip(pairs, tops))
            logs.append(high + jnp.log(total))
        targets = []
        for i in range(4):
            three = jnp.concatenate([posb[i, pl.ds(zh * 3 + t, 1), :] for t in range(3)], axis=1)
            targets.append(three[:, g * QUARTER : (g + 1) * QUARTER])
        for half in (0, 1):
            two = slice(half * 2, half * 2 + 2)
            logs_of[g, half] = jnp.concatenate(logs[two], axis=1)
            targets_of[g, half] = jnp.concatenate(targets[two], axis=1)

    def normalise(g, half):
        columns = slice(half * HALF, (half + 1) * HALF)
        log_total, targets = logs_of[g, half], targets_of[g, half]

        def normal(j, carry):
            rows = pl.ds(pl.multiple_of(j * QUARTER, 16), QUARTER)
            owner = (lax.rem(zl + lax.div(j, 2), 4) * 4 + x) * 2 + lax.rem(j, 2)
            ids = lax.broadcasted_iota(jnp.int32, (QUARTER, HALF), 0) + (owner * 768 + y * QUARTER)
            e = jnp.exp(sc[g, rows, columns] - log_total)
            sg[g, rows, columns] = jnp.where(ids == targets, e - 1.0, e).astype(BF16)
            return carry

        lax.fori_loop(0, 8, normal, 0)

    def query_gradients(g, half):
        r = lax.dot_general(
            sg[g, :, half * HALF : (half + 1) * HALF], wide(pb), TN, preferred_element_type=F32
        )
        pair = pl.ds(half * 2, 2)
        for k in (1, 3, 2, 0):
            columns = slice(k * 256, (k + 1) * 256)
            for i in range(2):
                part_a = r[i * QUARTER : i * QUARTER + EIGHTH, columns]
                part_b = r[i * QUARTER + EIGHTH : (i + 1) * QUARTER, columns]
                if half or i:
                    da[g, half * 2 + i, k] = part_a.astype(BF16)
                else:
                    own_a[g, k] = part_a
                if k:
                    db[g, k, half * 2 + i] = part_b.astype(BF16)
                else:
                    own_b[g, half * 2 + i] = part_b
            if k:
                send(db.at[g, k, pair], rb.at[g, -k % 4, pair], ("b", g), dy=k)
        for i in (3, 2) if half else (1,):
            send(da.at[g, i], ra.at[g, -i % 4], ("a", g), dx=i)

    def passages(s):
        rows = slice(s * HALF, (s + 1) * HALF)
        r = jnp.dot(
            jnp.concatenate([sg[g, rows, :] for g in range(2)], axis=1),
            jnp.concatenate([wide(qb, g) for g in range(2)], axis=0),
            preferred_element_type=F32,
        )
        for k in range(4):
            for i in range(2):
                for h in range(2):
                    column = k * 256 + h * 128
                    dps[s, i, h, k] = r[i * QUARTER : (i + 1) * QUARTER, column : column + 128]
        send(dps.at[s, oc], dpr.at[s], ("half", s), "half", dc=1)

    def half_arrived(*ss):
        for s in ss:
            arrived(("half", s), dpr.at[s])

    def both(dz, k):
        h = half_of(dz)
        return dps[dz % 4, c, h, k] + dpr[dz % 4, h, k]

    def add_on(way, n, sub, first=False):
        dz = (4 - n) if way == 0 else (4 + n)
        for i in range(2):
            v = both(dz, sub * 2 + i)
            if not first:
                v = v + rf[way, n, sub, i].astype(F32)
            sf[way, n, sub, i] = v.astype(BF16)
        send(sf.at[way, n, sub], rf.at[way, n + 1, sub], ("sum", way, n + 1, sub), "sum", dz=1 - 2 * way)

    def sum_arrived(way, n, sub):
        arrived(("sum", way, n, sub), rf.at[way, n, sub])

    def step(n):
        for way, sub in ((0, 1), (1, 0), (0, 0), (1, 1)):
            sum_arrived(way, n, sub)
            add_on(way, n, sub)

    def second_stage(g):
        arrived(("a", g), ra.at[g, pl.ds(1, 3)])
        arrived(("b", g), rb.at[g, pl.ds(1, 3)])
        for k in (1, 3, 2, 0):
            va = own_a[g, k] + sum(ra[g, i, k].astype(F32) for i in (1, 2, 3))
            vb = own_b[g, k] + sum(rb[g, i, k].astype(F32) for i in (1, 2, 3))
            if k:
                s2a[g, k] = va.astype(BF16)
                send(s2a.at[g, k], r2a.at[g, -k % 4], ("a2", g), dy=k)
                s2b[g, k] = vb.astype(BF16)
                send(s2b.at[g, k], r2b.at[g, -k % 4], ("b2", g), dx=k)
            else:
                own_a[g, 0] = va
                own_b[g, 0] = vb

    def third_stage(g):
        arrived(("a2", g), r2a.at[g, pl.ds(1, 3)])
        arrived(("b2", g), r2b.at[g, pl.ds(1, 3)])
        fa = own_a[g, 0] + sum(r2a[g, k].astype(F32) for k in (1, 2, 3))
        fb = own_b[g, 0] + sum(r2b[g, k].astype(F32) for k in (1, 2, 3))
        for h in range(2):
            zs[h, g, 0:EIGHTH, :] = fa[:, h * 128 : (h + 1) * 128].astype(BF16)
            zs[h, g, EIGHTH:QUARTER, :] = fb[:, h * 128 : (h + 1) * 128].astype(BF16)
        send(zs.at[oz, g], zr.at[g], ("last", g), dz=4)
        oq[pl.ds(pl.multiple_of(zh * HALF + g * QUARTER, 16), QUARTER), :] = zs[zh, g]

    normaliser(0)
    for half in (1, 0):
        normalise(0, half)
        query_gradients(0, half)
    normaliser(1)
    normalise(1, 1)
    normalise(1, 0)
    passages(0)
    passages(3)
    half_arrived(0)
    add_on(0, 0, 0, True)
    add_on(1, 0, 1, True)
    query_gradients(1, 1)
    half_arrived(3)
    add_on(0, 1, 1, True)
    query_gradients(1, 0)
    passages(1)
    passages(2)
    half_arrived(1)
    add_on(1, 1, 0, True)
    for way, sub in ((0, 0), (1, 1)):
        sum_arrived(way, 1, sub)
        add_on(way, 1, sub)
    half_arrived(2)
    second_stage(0)
    step(2)
    step(3)
    second_stage(1)
    third_stage(0)
    third_stage(1)

    for way, sub in ((0, 1), (1, 0), (0, 0), (1, 1)):
        sum_arrived(way, 4, sub)
    for k in (1, 3, 2, 0):
        v = both(0, k) + rf[0, 4, k // 2, k % 2].astype(F32) + rf[1, 4, k // 2, k % 2].astype(F32)
        if k:
            sy[k] = v.astype(BF16)
            send(sy.at[k], ry.at[-k % 4], "widths", dy=k)
        else:
            op[pl.ds(pl.multiple_of(y * QUARTER, 16), QUARTER), :] = v.astype(BF16)
    arrived("widths", ry.at[pl.ds(1, 3)])
    for k in (1, 2, 3):
        op[pl.ds(pl.multiple_of(lax.rem(y + k, 4) * QUARTER, 16), QUARTER), :] = ry[k]
    for g in (0, 1):
        arrived(("last", g), zr.at[g])
        oq[pl.ds(pl.multiple_of(oz * HALF + g * QUARTER, 16), QUARTER), :] = zr[g]
    rest = {
        "spread": pb.at[pl.ds(0, 3), 0, pl.ds(0, QUARTER)],
        "ring": pb.at[:, 0, pl.ds(0, 1344)],
        "core": pb.at[:, 0],
        ("share", 0): qb.at[pl.ds(0, 3), 0, 0],
        ("share", 1): qb.at[pl.ds(0, 3), 0, 0],
        "pos": posb.at[pl.ds(1, 3)],
        ("second", 0, "both"): qb.at[pl.ds(0, 3), 0, :, pl.ds(0, 576)],
        ("second", 1, 0): qb.at[pl.ds(0, 3), 0, pl.ds(0, 1), pl.ds(0, 576)],
        ("second", 1, 1): qb.at[pl.ds(0, 3), 0, pl.ds(0, 1), pl.ds(0, 576)],
        "half": dpr,
        "sum": pb.at[:, 0, pl.ds(0, 1344)],
        "widths": ry.at[pl.ds(1, 3)],
    }
    for g in (0, 1):
        rest["stats", g] = st.at[g, pl.ds(1, 15)]
        rest["a", g], rest["b", g] = ra.at[g, pl.ds(1, 3)], rb.at[g, pl.ds(1, 3)]
        rest["a2", g], rest["b2", g] = r2a.at[g, pl.ds(1, 3)], r2b.at[g, pl.ds(1, 3)]
    for out, dsts in leaving.items():
        ref = dsts[0] if len(dsts) == 1 else rest[out]
        size = lambda r: math.prod(r.shape) * r.dtype.itemsize
        assert size(ref) == sum(size(d) for d in dsts), out
        left(out, ref)
    assert (len(arrivals), len(departures)) == (ARRIVALS, DEPARTURES), (len(arrivals), len(departures))


def local(queries, passages, positive):
    vmem = pl.BlockSpec(memory_space=pltpu.VMEM)
    shapes = [
        ((4, QUARTER, 128), BF16),
        ((768, 128), BF16),
        ((6, 128), jnp.int32),
        ((4, 2, 2, GROUP, 128), BF16),
        ((4, 2, BLOCK, 128), BF16),
        ((4, 6, 128), jnp.int32),
        ((2, BLOCK, GROUP), F32),
        ((2, BLOCK, GROUP), BF16),
        ((2, 16, 4, 2, QUARTER), F32),
        ((2, 4, 4, EIGHTH, 256), BF16),
        ((2, 4, 4, EIGHTH, 256), BF16),
        ((2, 4, EIGHTH, 256), F32),
        ((2, 4, EIGHTH, 256), F32),
        ((2, 4, 4, EIGHTH, 256), BF16),
        ((2, 4, 4, EIGHTH, 256), BF16),
        ((2, 4, EIGHTH, 256), BF16),
        ((2, 4, EIGHTH, 256), BF16),
        ((2, 4, EIGHTH, 256), BF16),
        ((2, 4, EIGHTH, 256), BF16),
        ((2, 2, QUARTER, 128), BF16),
        ((2, QUARTER, 128), BF16),
        ((4, 2, 2, 4, QUARTER, 128), F32),
        ((4, 2, 4, QUARTER, 128), F32),
        ((2, 4, 2, 2, QUARTER, 128), BF16),
        ((2, 5, 2, 2, QUARTER, 128), BF16),
        ((4, QUARTER, 128), BF16),
        ((4, QUARTER, 128), BF16),
    ]
    return pl.pallas_call(
        kernel,
        out_shape=(pltpu.VMEM((768, 128), BF16), pltpu.VMEM((768, 128), BF16)),
        in_specs=[pl.BlockSpec(memory_space=pl.ANY)] * 3,
        out_specs=(vmem, vmem),
        scratch_shapes=[pltpu.VMEM(s, t) for s, t in shapes]
        + [pltpu.SemaphoreType.DMA((n,)) for n in (DEPARTURES, ARRIVALS, 3)],
        compiler_params=pltpu.CompilerParams(
            collective_id=0, has_side_effects=True, vmem_limit_bytes=62 * 2**20
        ),
    )(queries.reshape(4, QUARTER, 128), passages, positive.reshape(6, 128))


def solution(mesh):
    finer = Mesh(mesh.devices.reshape(4, 4, 2, 2, 4), ("zl", "x", "c", "zh", "y"))
    dp, mp = ("zl", "x", "c"), ("zh", "y")
    return jax.shard_map(
        local,
        mesh=finer,
        in_specs=(P(dp, mp), P(dp, mp), P(dp)),
        out_specs=(P(dp, mp), P(dp, mp)),
        check_vma=False,
    )
```

```python
import functools
import math

import jax
import jax.numpy as jnp
from jax import lax
from jax.experimental import pallas as pl
from jax.experimental.pallas import tpu as pltpu
from jax.sharding import Mesh
from jax.sharding import PartitionSpec as P

BF16, F32 = jnp.bfloat16, jnp.float32
D = 1024
SCALE = 3.0 / math.sqrt(D)
EIGHTH, QUARTER, HALF = 96, 192, 384
BLOCK = 1536
GROUP = 768
ARRIVALS, DEPARTURES = 73, 25
NT = (((1,), (1,)), ((), ()))
TN = (((0,), (0,)), ((), ()))


def place(dx=0, dy=0, dz=0, dc=0):
    z = lax.rem(lax.axis_index("zh") * 4 + lax.axis_index("zl") + dz + 8, 8)
    return {
        "zl": lax.rem(z, 4),
        "x": lax.rem(lax.axis_index("x") + dx + 4, 4),
        "c": lax.rem(lax.axis_index("c") + dc, 2),
        "zh": lax.div(z, 4),
        "y": lax.rem(lax.axis_index("y") + dy + 4, 4),
    }


def kernel(
    q_hbm, p_hbm, pos_hbm, oq, op,
    q, p, pos, qb, pb, posb, sc, sg, st,
    da, db, own_a, own_b, ra, rb, s2a, s2b, r2a, r2b, zs, zr,
    dps, dpr, sf, rf, sy, ry,
    ssem, rsem, isem,
):
    x, y, c, zl, zh = (lax.axis_index(a) for a in ("x", "y", "c", "zl", "zh"))
    oc = 1 - c
    oz = 1 - zh
    arrivals, departures, leaving = {}, {}, {}

    def send(src, dst, tag, out=None, **where):
        out = tag if out is None else out
        copy = pltpu.make_async_remote_copy(
            src_ref=src, dst_ref=dst,
            send_sem=ssem.at[departures.setdefault(out, len(departures))],
            recv_sem=rsem.at[arrivals.setdefault(tag, len(arrivals))],
            device_id=place(**where), device_id_type=pl.DeviceIdType.MESH,
        )
        copy.start()
        leaving.setdefault(out, []).append(dst)

    def arrived(tag, ref):
        pltpu.make_async_copy(ref, ref, rsem.at[arrivals[tag]]).wait()

    def left(out, ref):
        pltpu.make_async_copy(ref, ref, ssem.at[departures[out]]).wait()

    def half_of(dz):
        return lax.div(lax.rem(zh * 4 + zl + dz, 8), 4)

    plane = [(dx, dy) for dx in range(4) for dy in range(4) if dx or dy]
    peers = [dict(dx=dx, dy=dy) for dx, dy in plane]
    peers += [dict(dz=1), dict(dz=-1), dict(dz=4), dict(dc=1)]
    inputs = [
        pltpu.make_async_copy(a, b, isem.at[k]) for k, (a, b) in enumerate(((q_hbm, q), (p_hbm, p), (pos_hbm, pos)))
    ]
    for copy in inputs:
        copy.start()
    barrier = pltpu.get_barrier_semaphore()
    for where in peers:
        pl.semaphore_signal(barrier, inc=1, device_id=place(**where), device_id_type=pl.DeviceIdType.MESH)
    pl.semaphore_wait(barrier, len(peers))

    for copy in inputs:
        copy.wait()

    mine = pl.ds(pl.multiple_of(c * QUARTER, 16), QUARTER)
    send(q.at[pl.ds(oz * 2, 2)], qb.at[0, zh, :, pl.ds(0, QUARTER)], "swap", dz=4)
    for d in (1, 3, 2):
        rows = pl.ds(pl.multiple_of(lax.rem(y + d, 4) * QUARTER, 16), QUARTER)
        send(p.at[rows], pb.at[-d % 4, zh, mine], ("spread", -d % 4), "spread", dy=d)

    def share(src, h, tag):
        for d in (1, 3, 2):
            send(src, qb.at[-d % 4, h, :, pl.ds(0, QUARTER)], ("y", -d % 4, tag), ("share", tag), dy=d)
            send(src, qb.at[0, h, :, pl.ds((-d % 4) * QUARTER, QUARTER)], ("x", -d % 4, tag), ("share", tag), dx=d)

    share(q.at[pl.ds(zh * 2, 2)], zh, 0)
    for d in (1, 3, 2):
        send(pos, posb.at[-d % 4], "pos", dx=d)
    for g in (0, 1):
        qb[0, zh, g, 0:QUARTER, :] = q[zh * 2 + g]
    posb[0] = pos[...]
    pb[0, zh, mine, :] = p[pl.ds(pl.multiple_of(y * QUARTER, 16), QUARTER), :]

    def piece(dz, sub):
        rows = pl.ds(pl.multiple_of((dz % 4) * 2 * QUARTER + c * QUARTER, 16), QUARTER)
        ys = pl.ds(0, 4) if sub is None else pl.ds(sub * 2, 2)
        return ys, half_of(dz), rows

    def pass_on(dz, sub, step):
        ys, h, rows = piece(dz, sub)
        to = (dz - step) % 8
        to_rows = pl.ds(pl.multiple_of((to % 4) * 2 * QUARTER + c * QUARTER, 16), QUARTER)
        send(pb.at[ys, h, rows], pb.at[ys, h, to_rows], ("ring", to, sub), "ring", dz=step)

    def ring_arrived(dz, sub):
        arrived(("ring", dz, sub), pb.at[pl.ds(0, 2), 0, pl.ds(0, QUARTER)])

    def to_core(dz):
        ys, h, rows = piece(dz, None)
        send(pb.at[ys, h, rows], pb.at[ys, h, rows], ("core", dz), "core", dc=1)

    def core_arrived(*dzs):
        for dz in dzs:
            arrived(("core", dz), pb.at[:, 0, pl.ds(0, QUARTER)])

    def spread_arrived(*ds):
        for d in ds:
            arrived(("spread", d), pb.at[0, 0, pl.ds(0, QUARTER)])

    def groups_of(groups):
        return pl.ds(0, 2) if groups == "both" else pl.ds(groups, 1)

    def spread_y(k, tag, h, groups):
        gs, rows = groups_of(groups), pl.ds(0, EIGHTH)
        for d in (1, 3, 2):
            to_rows = pl.ds((-d % 4) * QUARTER, EIGHTH)
            send(qb.at[k, h, gs, rows], qb.at[k, h, gs, to_rows], ("second", tag, groups), dx=d)

    def spread_x(k, tag, h, groups):
        gs, rows = groups_of(groups), pl.ds(k * QUARTER + EIGHTH, EIGHTH)
        for d in (1, 3, 2):
            send(qb.at[0, h, gs, rows], qb.at[-d % 4, h, gs, rows], ("second", tag, groups), dy=d)

    def share_arrived(way, k, tag):
        arrived((way, k, tag), qb.at[0, 0, :, pl.ds(0, QUARTER)])

    def second_arrived(tag, groups):
        arrived(("second", tag, groups), qb.at[pl.ds(0, 3), 0, groups_of(groups), pl.ds(0, 576)])

    def hop(n):
        for sub in (0, 1):
            for dz, step in ((n, -1), (8 - n, 1)):
                ring_arrived(dz, sub)
                if n < 3 or (sub == 0) == (step == -1):
                    pass_on(dz, sub, step)
        to_core(n)
        to_core(8 - n)

    spread_arrived(1)
    pass_on(0, 0, 1)
    pass_on(0, 0, -1)
    spread_arrived(3, 2)
    pass_on(0, 1, 1)
    pass_on(0, 1, -1)
    to_core(0)
    share_arrived("x", 1, 0)
    spread_x(1, 0, zh, "both")
    share_arrived("y", 1, 0)
    spread_y(1, 0, zh, "both")
    arrived("swap", qb.at[0, 0, :, pl.ds(0, QUARTER)])
    share(qb.at[0, oz, :, pl.ds(0, QUARTER)], oz, 1)
    for k in (3, 2):
        share_arrived("x", k, 0)
        spread_x(k, 0, zh, "both")
        share_arrived("y", k, 0)
        spread_y(k, 0, zh, "both")
    hop(1)
    hop(2)
    for k in (1, 3, 2):
        share_arrived("x", k, 1)
        share_arrived("y", k, 1)
    for g in (0, 1):
        for k in (1, 3, 2):
            spread_x(k, 1, oz, g)
            spread_y(k, 1, oz, g)
    hop(3)
    arrived("pos", posb.at[pl.ds(1, 3)])
    second_arrived(0, "both")
    second_arrived(1, 0)

    def wide(ref, *at):
        return jnp.concatenate([ref[(k, h, *at)] for k in range(4) for h in range(2)], axis=1)

    best = {0: None, 1: None}

    def scores(g, n):
        rows = slice(n * HALF, (n + 1) * HALF)
        sc[g, rows, :] = lax.dot_general(wide(pb, rows), wide(qb, g), NT, preferred_element_type=F32) * SCALE

    def tally(g, n):
        s = sc[g, n * HALF : (n + 1) * HALF, :]
        high = jnp.max(s, axis=0, keepdims=True)
        if best[g] is None:
            best[g] = high, jnp.sum(jnp.exp(s - high), axis=0, keepdims=True)
        else:
            top, total = best[g]
            higher = jnp.maximum(top, high)
            total = total * jnp.exp(top - higher) + jnp.sum(jnp.exp(s - higher), axis=0, keepdims=True)
            best[g] = higher, total

    def publish(g):
        top, total = best[g]
        for i in range(4):
            st[g, 0, i, 0:1, :] = top[:, i * QUARTER : (i + 1) * QUARTER]
            st[g, 0, i, 1:2, :] = total[:, i * QUARTER : (i + 1) * QUARTER]
        for dx, dy in plane:
            send(st.at[g, 0], st.at[g, (-dx % 4) * 4 + (-dy % 4)], ("stats", g), dx=dx, dy=dy)

    core_arrived(2, 6)
    scores(0, 2)
    for sub in (0, 1):
        ring_arrived(4, sub)
    to_core(4)
    core_arrived(1, 5, 3, 7)
    scores(0, 1)
    tally(0, 2)
    scores(0, 3)
    tally(0, 1)
    core_arrived(0, 4)
    scores(0, 0)
    tally(0, 3)
    tally(0, 0)
    publish(0)
    second_arrived(1, 1)
    scores(1, 2)
    scores(1, 1)
    tally(1, 2)
    scores(1, 3)
    tally(1, 1)
    scores(1, 0)
    tally(1, 3)
    tally(1, 0)
    publish(1)

    logs_of, targets_of = {}, {}

    def normaliser(g):
        arrived(("stats", g), st.at[g, pl.ds(1, 15)])
        logs = []
        for i in range(4):
            pairs = [(k, (i - k // 4) % 4) for k in range(16)]
            tops = [st[g, k, n, 0:1, :] for k, n in pairs]
            high = functools.reduce(jnp.maximum, tops)
            total = sum(st[g, k, n, 1:2, :] * jnp.exp(t - high) for (k, n), t in zip(pairs, tops))
            logs.append(high + jnp.log(total))
        targets = []
        for i in range(4):
            three = jnp.concatenate([posb[i, pl.ds(zh * 3 + t, 1), :] for t in range(3)], axis=1)
            targets.append(three[:, g * QUARTER : (g + 1) * QUARTER])
        for half in (0, 1):
            two = slice(half * 2, half * 2 + 2)
            logs_of[g, half] = jnp.concatenate(logs[two], axis=1)
            targets_of[g, half] = jnp.concatenate(targets[two], axis=1)

    def normalise(g, half):
        columns = slice(half * HALF, (half + 1) * HALF)
        log_total, targets = logs_of[g, half], targets_of[g, half]

        def normal(j, carry):
            rows = pl.ds(pl.multiple_of(j * QUARTER, 16), QUARTER)
            owner = (lax.rem(zl + lax.div(j, 2), 4) * 4 + x) * 2 + lax.rem(j, 2)
            ids = lax.broadcasted_iota(jnp.int32, (QUARTER, HALF), 0) + (owner * 768 + y * QUARTER)
            e = jnp.exp(sc[g, rows, columns] - log_total)
            sg[g, rows, columns] = jnp.where(ids == targets, e - 1.0, e).astype(BF16)
            return carry

        lax.fori_loop(0, 8, normal, 0)

    def query_gradients(g, half):
        r = lax.dot_general(
            sg[g, :, half * HALF : (half + 1) * HALF], wide(pb), TN, preferred_element_type=F32
        )
        pair = pl.ds(half * 2, 2)
        for k in (1, 3, 2, 0):
            columns = slice(k * 256, (k + 1) * 256)
            for i in range(2):
                part_a = r[i * QUARTER : i * QUARTER + EIGHTH, columns]
                part_b = r[i * QUARTER + EIGHTH : (i + 1) * QUARTER, columns]
                if half or i:
                    da[g, half * 2 + i, k] = part_a.astype(BF16)
                else:
                    own_a[g, k] = part_a
                if k:
                    db[g, k, half * 2 + i] = part_b.astype(BF16)
                else:
                    own_b[g, half * 2 + i] = part_b
            if k:
                send(db.at[g, k, pair], rb.at[g, -k % 4, pair], ("b", g), dy=k)
        for i in (3, 2) if half else (1,):
            send(da.at[g, i], ra.at[g, -i % 4], ("a", g), dx=i)

    def passages(s):
        rows = slice(s * HALF, (s + 1) * HALF)
        r = jnp.dot(
            jnp.concatenate([sg[g, rows, :] for g in range(2)], axis=1),
            jnp.concatenate([wide(qb, g) for g in range(2)], axis=0),
            preferred_element_type=F32,
        )
        for k in range(4):
            for i in range(2):
                for h in range(2):
                    column = k * 256 + h * 128
                    dps[s, i, h, k] = r[i * QUARTER : (i + 1) * QUARTER, column : column + 128]
        send(dps.at[s, oc], dpr.at[s], ("half", s), "half", dc=1)

    def half_arrived(*ss):
        for s in ss:
            arrived(("half", s), dpr.at[s])

    def both(dz, k):
        h = half_of(dz)
        return dps[dz % 4, c, h, k] + dpr[dz % 4, h, k]

    def add_on(way, n, sub, first=False):
        dz = (4 - n) if way == 0 else (4 + n)
        for i in range(2):
            v = both(dz, sub * 2 + i)
            if not first:
                v = v + rf[way, n, sub, i].astype(F32)
            sf[way, n, sub, i] = v.astype(BF16)
        send(sf.at[way, n, sub], rf.at[way, n + 1, sub], ("sum", way, n + 1, sub), "sum", dz=1 - 2 * way)

    def sum_arrived(way, n, sub):
        arrived(("sum", way, n, sub), rf.at[way, n, sub])

    def step(n):
        for way, sub in ((0, 1), (1, 0), (0, 0), (1, 1)):
            sum_arrived(way, n, sub)
            add_on(way, n, sub)

    def second_stage(g):
        arrived(("a", g), ra.at[g, pl.ds(1, 3)])
        arrived(("b", g), rb.at[g, pl.ds(1, 3)])
        for k in (1, 3, 2, 0):
            va = own_a[g, k] + sum(ra[g, i, k].astype(F32) for i in (1, 2, 3))
            vb = own_b[g, k] + sum(rb[g, i, k].astype(F32) for i in (1, 2, 3))
            if k:
                s2a[g, k] = va.astype(BF16)
                send(s2a.at[g, k], r2a.at[g, -k % 4], ("a2", g), dy=k)
                s2b[g, k] = vb.astype(BF16)
                send(s2b.at[g, k], r2b.at[g, -k % 4], ("b2", g), dx=k)
            else:
                own_a[g, 0] = va
                own_b[g, 0] = vb

    def third_stage(g):
        arrived(("a2", g), r2a.at[g, pl.ds(1, 3)])
        arrived(("b2", g), r2b.at[g, pl.ds(1, 3)])
        fa = own_a[g, 0] + sum(r2a[g, k].astype(F32) for k in (1, 2, 3))
        fb = own_b[g, 0] + sum(r2b[g, k].astype(F32) for k in (1, 2, 3))
        for h in range(2):
            zs[h, g, 0:EIGHTH, :] = fa[:, h * 128 : (h + 1) * 128].astype(BF16)
            zs[h, g, EIGHTH:QUARTER, :] = fb[:, h * 128 : (h + 1) * 128].astype(BF16)
        send(zs.at[oz, g], zr.at[g], ("last", g), dz=4)
        oq[pl.ds(pl.multiple_of(zh * HALF + g * QUARTER, 16), QUARTER), :] = zs[zh, g]

    normaliser(0)
    normalise(0, 1)
    query_gradients(0, 1)
    normalise(0, 0)
    normaliser(1)
    normalise(1, 1)
    normalise(1, 0)
    passages(0)
    query_gradients(0, 0)
    passages(3)
    half_arrived(0)
    add_on(0, 0, 0, True)
    add_on(1, 0, 1, True)
    passages(1)
    query_gradients(1, 1)
    half_arrived(3, 1)
    add_on(0, 1, 1, True)
    add_on(1, 1, 0, True)
    passages(2)
    for way, sub in ((0, 0), (1, 1)):
        sum_arrived(way, 1, sub)
        add_on(way, 1, sub)
    query_gradients(1, 0)
    second_stage(0)
    half_arrived(2)
    step(2)
    step(3)
    second_stage(1)
    third_stage(0)
    third_stage(1)

    def last_step(k):
        v = both(0, k) + rf[0, 4, k // 2, k % 2].astype(F32) + rf[1, 4, k // 2, k % 2].astype(F32)
        if k:
            sy[k] = v.astype(BF16)
            send(sy.at[k], ry.at[-k % 4], "widths", dy=k)
        else:
            op[pl.ds(pl.multiple_of(y * QUARTER, 16), QUARTER), :] = v.astype(BF16)

    for way, sub in ((0, 1), (1, 0), (0, 0)):
        sum_arrived(way, 4, sub)
    last_step(1)
    sum_arrived(1, 4, 1)
    for k in (3, 2, 0):
        last_step(k)
    arrived("widths", ry.at[pl.ds(1, 3)])
    for k in (1, 2, 3):
        op[pl.ds(pl.multiple_of(lax.rem(y + k, 4) * QUARTER, 16), QUARTER), :] = ry[k]
    for g in (0, 1):
        arrived(("last", g), zr.at[g])
        oq[pl.ds(pl.multiple_of(oz * HALF + g * QUARTER, 16), QUARTER), :] = zr[g]
    rest = {
        "spread": pb.at[pl.ds(0, 3), 0, pl.ds(0, QUARTER)],
        "ring": pb.at[:, 0, pl.ds(0, 1344)],
        "core": pb.at[:, 0],
        ("share", 0): qb.at[pl.ds(0, 3), 0, 0],
        ("share", 1): qb.at[pl.ds(0, 3), 0, 0],
        "pos": posb.at[pl.ds(1, 3)],
        ("second", 0, "both"): qb.at[pl.ds(0, 3), 0, :, pl.ds(0, 576)],
        ("second", 1, 0): qb.at[pl.ds(0, 3), 0, pl.ds(0, 1), pl.ds(0, 576)],
        ("second", 1, 1): qb.at[pl.ds(0, 3), 0, pl.ds(0, 1), pl.ds(0, 576)],
        "half": dpr,
        "sum": pb.at[:, 0, pl.ds(0, 1344)],
        "widths": ry.at[pl.ds(1, 3)],
    }
    for g in (0, 1):
        rest["stats", g] = st.at[g, pl.ds(1, 15)]
        rest["a", g], rest["b", g] = ra.at[g, pl.ds(1, 3)], rb.at[g, pl.ds(1, 3)]
        rest["a2", g], rest["b2", g] = r2a.at[g, pl.ds(1, 3)], r2b.at[g, pl.ds(1, 3)]
    for out, dsts in leaving.items():
        ref = dsts[0] if len(dsts) == 1 else rest[out]
        size = lambda r: math.prod(r.shape) * r.dtype.itemsize
        assert size(ref) == sum(size(d) for d in dsts), out
        left(out, ref)
    assert (len(arrivals), len(departures)) == (ARRIVALS, DEPARTURES), (len(arrivals), len(departures))


def local(queries, passages, positive):
    vmem = pl.BlockSpec(memory_space=pltpu.VMEM)
    shapes = [
        ((4, QUARTER, 128), BF16),
        ((768, 128), BF16),
        ((6, 128), jnp.int32),
        ((4, 2, 2, GROUP, 128), BF16),
        ((4, 2, BLOCK, 128), BF16),
        ((4, 6, 128), jnp.int32),
        ((2, BLOCK, GROUP), F32),
        ((2, BLOCK, GROUP), BF16),
        ((2, 16, 4, 2, QUARTER), F32),
        ((2, 4, 4, EIGHTH, 256), BF16),
        ((2, 4, 4, EIGHTH, 256), BF16),
        ((2, 4, EIGHTH, 256), F32),
        ((2, 4, EIGHTH, 256), F32),
        ((2, 4, 4, EIGHTH, 256), BF16),
        ((2, 4, 4, EIGHTH, 256), BF16),
        ((2, 4, EIGHTH, 256), BF16),
        ((2, 4, EIGHTH, 256), BF16),
        ((2, 4, EIGHTH, 256), BF16),
        ((2, 4, EIGHTH, 256), BF16),
        ((2, 2, QUARTER, 128), BF16),
        ((2, QUARTER, 128), BF16),
        ((4, 2, 2, 4, QUARTER, 128), F32),
        ((4, 2, 4, QUARTER, 128), F32),
        ((2, 4, 2, 2, QUARTER, 128), BF16),
        ((2, 5, 2, 2, QUARTER, 128), BF16),
        ((4, QUARTER, 128), BF16),
        ((4, QUARTER, 128), BF16),
    ]
    return pl.pallas_call(
        kernel,
        out_shape=(pltpu.VMEM((768, 128), BF16), pltpu.VMEM((768, 128), BF16)),
        in_specs=[pl.BlockSpec(memory_space=pl.ANY)] * 3,
        out_specs=(vmem, vmem),
        scratch_shapes=[pltpu.VMEM(s, t) for s, t in shapes]
        + [pltpu.SemaphoreType.DMA((n,)) for n in (DEPARTURES, ARRIVALS, 3)],
        compiler_params=pltpu.CompilerParams(
            collective_id=0, has_side_effects=True, vmem_limit_bytes=62 * 2**20
        ),
    )(queries.reshape(4, QUARTER, 128), passages, positive.reshape(6, 128))


def solution(mesh):
    finer = Mesh(mesh.devices.reshape(4, 4, 2, 2, 4), ("zl", "x", "c", "zh", "y"))
    dp, mp = ("zl", "x", "c"), ("zh", "y")
    return jax.shard_map(
        local,
        mesh=finer,
        in_specs=(P(dp, mp), P(dp, mp), P(dp)),
        out_specs=(P(dp, mp), P(dp, mp)),
        check_vma=False,
    )
```

```python
import functools
import math

import jax
import jax.numpy as jnp
from jax import lax
from jax.experimental import pallas as pl
from jax.experimental.pallas import tpu as pltpu
from jax.sharding import Mesh
from jax.sharding import PartitionSpec as P

BF16, F32 = jnp.bfloat16, jnp.float32
D = 1024
SCALE = 3.0 / math.sqrt(D)
EIGHTH, QUARTER, HALF = 96, 192, 384
BLOCK = 1536
GROUP = 768
ARRIVALS, DEPARTURES = 73, 25
NT = (((1,), (1,)), ((), ()))
TN = (((0,), (0,)), ((), ()))


def place(dx=0, dy=0, dz=0, dc=0):
    z = lax.rem(lax.axis_index("zh") * 4 + lax.axis_index("zl") + dz + 8, 8)
    return {
        "zl": lax.rem(z, 4),
        "x": lax.rem(lax.axis_index("x") + dx + 4, 4),
        "c": lax.rem(lax.axis_index("c") + dc, 2),
        "zh": lax.div(z, 4),
        "y": lax.rem(lax.axis_index("y") + dy + 4, 4),
    }


def kernel(
    q_hbm, p_hbm, pos_hbm, out,
    q, p, pos, qb, pb, posb, sc, sg, st,
    da, db, own_a, own_b, ra, rb, s2a, s2b, r2a, r2b, zs, zr,
    dps, dpr, sf, rf, sy, ry,
    ssem, rsem, isem,
):
    x, y, c, zl, zh = (lax.axis_index(a) for a in ("x", "y", "c", "zl", "zh"))
    oc = 1 - c
    oz = 1 - zh
    arrivals, departures, leaving = {}, {}, {}

    def send(src, dst, tag, out=None, **where):
        out = tag if out is None else out
        copy = pltpu.make_async_remote_copy(
            src_ref=src, dst_ref=dst,
            send_sem=ssem.at[departures.setdefault(out, len(departures))],
            recv_sem=rsem.at[arrivals.setdefault(tag, len(arrivals))],
            device_id=place(**where), device_id_type=pl.DeviceIdType.MESH,
        )
        copy.start()
        leaving.setdefault(out, []).append(dst)

    def arrived(tag, ref):
        pltpu.make_async_copy(ref, ref, rsem.at[arrivals[tag]]).wait()

    def left(out, ref):
        pltpu.make_async_copy(ref, ref, ssem.at[departures[out]]).wait()

    def half_of(dz):
        return lax.div(lax.rem(zh * 4 + zl + dz, 8), 4)

    plane = [(dx, dy) for dx in range(4) for dy in range(4) if dx or dy]
    peers = [dict(dx=dx, dy=dy) for dx, dy in plane]
    peers += [dict(dz=1), dict(dz=-1), dict(dz=4), dict(dc=1)]
    inputs = [
        pltpu.make_async_copy(a, b, isem.at[k]) for k, (a, b) in enumerate(((q_hbm, q), (p_hbm, p), (pos_hbm, pos)))
    ]
    for copy in inputs:
        copy.start()
    barrier = pltpu.get_barrier_semaphore()
    for where in peers:
        pl.semaphore_signal(barrier, inc=1, device_id=place(**where), device_id_type=pl.DeviceIdType.MESH)
    pl.semaphore_wait(barrier, len(peers))

    for copy in inputs:
        copy.wait()

    mine = pl.ds(pl.multiple_of(c * QUARTER, 16), QUARTER)
    send(q.at[pl.ds(oz * 2, 2)], qb.at[0, zh, :, pl.ds(0, QUARTER)], "swap", dz=4)
    for d in (1, 3, 2):
        rows = pl.ds(pl.multiple_of(lax.rem(y + d, 4) * QUARTER, 16), QUARTER)
        send(p.at[rows], pb.at[-d % 4, zh, mine], ("spread", -d % 4), "spread", dy=d)

    def share(src, h, tag):
        for d in (1, 3, 2):
            send(src, qb.at[-d % 4, h, :, pl.ds(0, QUARTER)], ("y", -d % 4, tag), ("share", tag), dy=d)
            send(src, qb.at[0, h, :, pl.ds((-d % 4) * QUARTER, QUARTER)], ("x", -d % 4, tag), ("share", tag), dx=d)

    share(q.at[pl.ds(zh * 2, 2)], zh, 0)
    for d in (1, 3, 2):
        send(pos, posb.at[-d % 4], "pos", dx=d)
    for g in (0, 1):
        qb[0, zh, g, 0:QUARTER, :] = q[zh * 2 + g]
    posb[0] = pos[...]
    pb[0, zh, mine, :] = p[pl.ds(pl.multiple_of(y * QUARTER, 16), QUARTER), :]

    def piece(dz, sub):
        rows = pl.ds(pl.multiple_of((dz % 4) * 2 * QUARTER + c * QUARTER, 16), QUARTER)
        ys = pl.ds(0, 4) if sub is None else pl.ds(sub * 2, 2)
        return ys, half_of(dz), rows

    def pass_on(dz, sub, step):
        ys, h, rows = piece(dz, sub)
        to = (dz - step) % 8
        to_rows = pl.ds(pl.multiple_of((to % 4) * 2 * QUARTER + c * QUARTER, 16), QUARTER)
        send(pb.at[ys, h, rows], pb.at[ys, h, to_rows], ("ring", to, sub), "ring", dz=step)

    def ring_arrived(dz, sub):
        arrived(("ring", dz, sub), pb.at[pl.ds(0, 2), 0, pl.ds(0, QUARTER)])

    def to_core(dz):
        ys, h, rows = piece(dz, None)
        send(pb.at[ys, h, rows], pb.at[ys, h, rows], ("core", dz), "core", dc=1)

    def core_arrived(*dzs):
        for dz in dzs:
            arrived(("core", dz), pb.at[:, 0, pl.ds(0, QUARTER)])

    def spread_arrived(*ds):
        for d in ds:
            arrived(("spread", d), pb.at[0, 0, pl.ds(0, QUARTER)])

    def groups_of(groups):
        return pl.ds(0, 2) if groups == "both" else pl.ds(groups, 1)

    def spread_y(k, tag, h, groups):
        gs, rows = groups_of(groups), pl.ds(0, EIGHTH)
        for d in (1, 3, 2):
            to_rows = pl.ds((-d % 4) * QUARTER, EIGHTH)
            send(qb.at[k, h, gs, rows], qb.at[k, h, gs, to_rows], ("second", tag, groups), dx=d)

    def spread_x(k, tag, h, groups):
        gs, rows = groups_of(groups), pl.ds(k * QUARTER + EIGHTH, EIGHTH)
        for d in (1, 3, 2):
            send(qb.at[0, h, gs, rows], qb.at[-d % 4, h, gs, rows], ("second", tag, groups), dy=d)

    def share_arrived(way, k, tag):
        arrived((way, k, tag), qb.at[0, 0, :, pl.ds(0, QUARTER)])

    def second_arrived(tag, groups):
        arrived(("second", tag, groups), qb.at[pl.ds(0, 3), 0, groups_of(groups), pl.ds(0, 576)])

    def hop(n):
        for sub in (0, 1):
            for dz, step in ((n, -1), (8 - n, 1)):
                ring_arrived(dz, sub)
                if n < 3 or (sub == 0) == (step == -1):
                    pass_on(dz, sub, step)
        to_core(n)
        to_core(8 - n)

    spread_arrived(1)
    pass_on(0, 0, 1)
    pass_on(0, 0, -1)
    spread_arrived(3, 2)
    pass_on(0, 1, 1)
    pass_on(0, 1, -1)
    to_core(0)
    share_arrived("x", 1, 0)
    spread_x(1, 0, zh, "both")
    share_arrived("y", 1, 0)
    spread_y(1, 0, zh, "both")
    arrived("swap", qb.at[0, 0, :, pl.ds(0, QUARTER)])
    share(qb.at[0, oz, :, pl.ds(0, QUARTER)], oz, 1)
    for k in (3, 2):
        share_arrived("x", k, 0)
        spread_x(k, 0, zh, "both")
        share_arrived("y", k, 0)
        spread_y(k, 0, zh, "both")
    hop(1)
    hop(2)
    for k in (1, 3, 2):
        share_arrived("x", k, 1)
        share_arrived("y", k, 1)
    for g in (0, 1):
        for k in (1, 3, 2):
            spread_x(k, 1, oz, g)
            spread_y(k, 1, oz, g)
    hop(3)
    arrived("pos", posb.at[pl.ds(1, 3)])
    second_arrived(0, "both")
    second_arrived(1, 0)

    def wide(ref, *at):
        return jnp.concatenate([ref[(k, h, *at)] for k in range(4) for h in range(2)], axis=1)

    best = {0: None, 1: None}

    def scores(g, n):
        rows = slice(n * HALF, (n + 1) * HALF)
        sc[g, rows, :] = lax.dot_general(wide(pb, rows), wide(qb, g), NT, preferred_element_type=F32) * SCALE

    def tally(g, n):
        s = sc[g, n * HALF : (n + 1) * HALF, :]
        high = jnp.max(s, axis=0, keepdims=True)
        if best[g] is None:
            best[g] = high, jnp.sum(jnp.exp(s - high), axis=0, keepdims=True)
        else:
            top, total = best[g]
            higher = jnp.maximum(top, high)
            total = total * jnp.exp(top - higher) + jnp.sum(jnp.exp(s - higher), axis=0, keepdims=True)
            best[g] = higher, total

    def publish(g):
        top, total = best[g]
        for i in range(4):
            st[g, 0, i, 0:1, :] = top[:, i * QUARTER : (i + 1) * QUARTER]
            st[g, 0, i, 1:2, :] = total[:, i * QUARTER : (i + 1) * QUARTER]
        for dx, dy in plane:
            send(st.at[g, 0], st.at[g, (-dx % 4) * 4 + (-dy % 4)], ("stats", g), dx=dx, dy=dy)

    core_arrived(2, 6)
    scores(0, 2)
    for sub in (0, 1):
        ring_arrived(4, sub)
    to_core(4)
    core_arrived(1, 5, 3, 7)
    scores(0, 1)
    tally(0, 2)
    scores(0, 3)
    tally(0, 1)
    core_arrived(0, 4)
    scores(0, 0)
    tally(0, 3)
    tally(0, 0)
    publish(0)
    second_arrived(1, 1)
    scores(1, 2)
    scores(1, 1)
    tally(1, 2)
    scores(1, 3)
    tally(1, 1)
    scores(1, 0)
    tally(1, 3)
    tally(1, 0)
    publish(1)

    logs_of, targets_of = {}, {}

    def normaliser(g):
        arrived(("stats", g), st.at[g, pl.ds(1, 15)])
        logs = []
        for i in range(4):
            pairs = [(k, (i - k // 4) % 4) for k in range(16)]
            tops = [st[g, k, n, 0:1, :] for k, n in pairs]
            high = functools.reduce(jnp.maximum, tops)
            total = sum(st[g, k, n, 1:2, :] * jnp.exp(t - high) for (k, n), t in zip(pairs, tops))
            logs.append(high + jnp.log(total))
        targets = []
        for i in range(4):
            three = jnp.concatenate([posb[i, pl.ds(zh * 3 + t, 1), :] for t in range(3)], axis=1)
            targets.append(three[:, g * QUARTER : (g + 1) * QUARTER])
        for half in (0, 1):
            two = slice(half * 2, half * 2 + 2)
            logs_of[g, half] = jnp.concatenate(logs[two], axis=1)
            targets_of[g, half] = jnp.concatenate(targets[two], axis=1)

    def normalise(g, half):
        columns = slice(half * HALF, (half + 1) * HALF)
        log_total, targets = logs_of[g, half], targets_of[g, half]

        def normal(j, carry):
            rows = pl.ds(pl.multiple_of(j * QUARTER, 16), QUARTER)
            owner = (lax.rem(zl + lax.div(j, 2), 4) * 4 + x) * 2 + lax.rem(j, 2)
            ids = lax.broadcasted_iota(jnp.int32, (QUARTER, HALF), 0) + (owner * 768 + y * QUARTER)
            e = jnp.exp(sc[g, rows, columns] - log_total)
            sg[g, rows, columns] = jnp.where(ids == targets, e - 1.0, e).astype(BF16)
            return carry

        lax.fori_loop(0, 8, normal, 0)

    def query_gradients(g, half):
        r = lax.dot_general(
            sg[g, :, half * HALF : (half + 1) * HALF], wide(pb), TN, preferred_element_type=F32
        )
        pair = pl.ds(half * 2, 2)
        for k in (1, 3, 2, 0):
            columns = slice(k * 256, (k + 1) * 256)
            for i in range(2):
                part_a = r[i * QUARTER : i * QUARTER + EIGHTH, columns]
                part_b = r[i * QUARTER + EIGHTH : (i + 1) * QUARTER, columns]
                if half or i:
                    da[g, half * 2 + i, k] = part_a.astype(BF16)
                else:
                    own_a[g, k] = part_a
                if k:
                    db[g, k, half * 2 + i] = part_b.astype(BF16)
                else:
                    own_b[g, half * 2 + i] = part_b
            if k:
                send(db.at[g, k, pair], rb.at[g, -k % 4, pair], ("b", g), dy=k)
        for i in (3, 2) if half else (1,):
            send(da.at[g, i], ra.at[g, -i % 4], ("a", g), dx=i)

    def passages(s):
        rows = slice(s * HALF, (s + 1) * HALF)
        r = jnp.dot(
            jnp.concatenate([sg[g, rows, :] for g in range(2)], axis=1),
            jnp.concatenate([wide(qb, g) for g in range(2)], axis=0),
            preferred_element_type=F32,
        )
        for k in range(4):
            for i in range(2):
                for h in range(2):
                    column = k * 256 + h * 128
                    dps[s, i, h, k] = r[i * QUARTER : (i + 1) * QUARTER, column : column + 128]
        send(dps.at[s, oc], dpr.at[s], ("half", s), "half", dc=1)

    def half_arrived(*ss):
        for s in ss:
            arrived(("half", s), dpr.at[s])

    def both(dz, k):
        h = half_of(dz)
        return dps[dz % 4, c, h, k] + dpr[dz % 4, h, k]

    def add_on(way, n, sub, first=False):
        dz = (4 - n) if way == 0 else (4 + n)
        for i in range(2):
            v = both(dz, sub * 2 + i)
            if not first:
                v = v + rf[way, n, sub, i].astype(F32)
            sf[way, n, sub, i] = v.astype(BF16)
        send(sf.at[way, n, sub], rf.at[way, n + 1, sub], ("sum", way, n + 1, sub), "sum", dz=1 - 2 * way)

    def sum_arrived(way, n, sub):
        arrived(("sum", way, n, sub), rf.at[way, n, sub])

    def step(n):
        for way, sub in ((0, 1), (1, 0), (0, 0), (1, 1)):
            sum_arrived(way, n, sub)
            add_on(way, n, sub)

    def second_stage(g):
        arrived(("a", g), ra.at[g, pl.ds(1, 3)])
        arrived(("b", g), rb.at[g, pl.ds(1, 3)])
        for k in (1, 3, 2, 0):
            va = own_a[g, k] + sum(ra[g, i, k].astype(F32) for i in (1, 2, 3))
            vb = own_b[g, k] + sum(rb[g, i, k].astype(F32) for i in (1, 2, 3))
            if k:
                s2a[g, k] = va.astype(BF16)
                send(s2a.at[g, k], r2a.at[g, -k % 4], ("a2", g), dy=k)
                s2b[g, k] = vb.astype(BF16)
                send(s2b.at[g, k], r2b.at[g, -k % 4], ("b2", g), dx=k)
            else:
                own_a[g, 0] = va
                own_b[g, 0] = vb

    def third_stage(g):
        arrived(("a2", g), r2a.at[g, pl.ds(1, 3)])
        arrived(("b2", g), r2b.at[g, pl.ds(1, 3)])
        fa = own_a[g, 0] + sum(r2a[g, k].astype(F32) for k in (1, 2, 3))
        fb = own_b[g, 0] + sum(r2b[g, k].astype(F32) for k in (1, 2, 3))
        for h in range(2):
            zs[h, g, 0:EIGHTH, :] = fa[:, h * 128 : (h + 1) * 128].astype(BF16)
            zs[h, g, EIGHTH:QUARTER, :] = fb[:, h * 128 : (h + 1) * 128].astype(BF16)
        send(zs.at[oz, g], zr.at[g], ("last", g), dz=4)
        out[0, pl.ds(pl.multiple_of(zh * HALF + g * QUARTER, 16), QUARTER), :] = zs[zh, g]

    normaliser(0)
    normalise(0, 1)
    query_gradients(0, 1)
    normalise(0, 0)
    normaliser(1)
    normalise(1, 1)
    normalise(1, 0)
    passages(0)
    query_gradients(0, 0)
    passages(3)
    half_arrived(0)
    add_on(0, 0, 0, True)
    add_on(1, 0, 1, True)
    passages(1)
    query_gradients(1, 1)
    half_arrived(3, 1)
    add_on(0, 1, 1, True)
    add_on(1, 1, 0, True)
    passages(2)
    for way, sub in ((0, 0), (1, 1)):
        sum_arrived(way, 1, sub)
        add_on(way, 1, sub)
    query_gradients(1, 0)
    second_stage(0)
    half_arrived(2)
    step(2)
    step(3)
    second_stage(1)
    third_stage(0)
    third_stage(1)

    def last_step(k):
        v = both(0, k) + rf[0, 4, k // 2, k % 2].astype(F32) + rf[1, 4, k // 2, k % 2].astype(F32)
        if k:
            sy[k] = v.astype(BF16)
            send(sy.at[k], ry.at[-k % 4], "widths", dy=k)
        else:
            out[1, pl.ds(pl.multiple_of(y * QUARTER, 16), QUARTER), :] = v.astype(BF16)

    for way, sub in ((0, 1), (1, 0), (0, 0)):
        sum_arrived(way, 4, sub)
    last_step(1)
    sum_arrived(1, 4, 1)
    for k in (3, 2, 0):
        last_step(k)
    arrived("widths", ry.at[pl.ds(1, 3)])
    for k in (1, 2, 3):
        out[1, pl.ds(pl.multiple_of(lax.rem(y + k, 4) * QUARTER, 16), QUARTER), :] = ry[k]
    for g in (0, 1):
        arrived(("last", g), zr.at[g])
        out[0, pl.ds(pl.multiple_of(oz * HALF + g * QUARTER, 16), QUARTER), :] = zr[g]
    rest = {
        "spread": pb.at[pl.ds(0, 3), 0, pl.ds(0, QUARTER)],
        "ring": pb.at[:, 0, pl.ds(0, 1344)],
        "core": pb.at[:, 0],
        ("share", 0): qb.at[pl.ds(0, 3), 0, 0],
        ("share", 1): qb.at[pl.ds(0, 3), 0, 0],
        "pos": posb.at[pl.ds(1, 3)],
        ("second", 0, "both"): qb.at[pl.ds(0, 3), 0, :, pl.ds(0, 576)],
        ("second", 1, 0): qb.at[pl.ds(0, 3), 0, pl.ds(0, 1), pl.ds(0, 576)],
        ("second", 1, 1): qb.at[pl.ds(0, 3), 0, pl.ds(0, 1), pl.ds(0, 576)],
        "half": dpr,
        "sum": pb.at[:, 0, pl.ds(0, 1344)],
        "widths": ry.at[pl.ds(1, 3)],
    }
    for g in (0, 1):
        rest["stats", g] = st.at[g, pl.ds(1, 15)]
        rest["a", g], rest["b", g] = ra.at[g, pl.ds(1, 3)], rb.at[g, pl.ds(1, 3)]
        rest["a2", g], rest["b2", g] = r2a.at[g, pl.ds(1, 3)], r2b.at[g, pl.ds(1, 3)]
    for out, dsts in leaving.items():
        ref = dsts[0] if len(dsts) == 1 else rest[out]
        size = lambda r: math.prod(r.shape) * r.dtype.itemsize
        assert size(ref) == sum(size(d) for d in dsts), out
        left(out, ref)
    assert (len(arrivals), len(departures)) == (ARRIVALS, DEPARTURES), (len(arrivals), len(departures))


def local(queries, passages, positive):
    vmem = pl.BlockSpec(memory_space=pltpu.VMEM)
    shapes = [
        ((4, QUARTER, 128), BF16),
        ((768, 128), BF16),
        ((6, 128), jnp.int32),
        ((4, 2, 2, GROUP, 128), BF16),
        ((4, 2, BLOCK, 128), BF16),
        ((4, 6, 128), jnp.int32),
        ((2, BLOCK, GROUP), F32),
        ((2, BLOCK, GROUP), BF16),
        ((2, 16, 4, 2, QUARTER), F32),
        ((2, 4, 4, EIGHTH, 256), BF16),
        ((2, 4, 4, EIGHTH, 256), BF16),
        ((2, 4, EIGHTH, 256), F32),
        ((2, 4, EIGHTH, 256), F32),
        ((2, 4, 4, EIGHTH, 256), BF16),
        ((2, 4, 4, EIGHTH, 256), BF16),
        ((2, 4, EIGHTH, 256), BF16),
        ((2, 4, EIGHTH, 256), BF16),
        ((2, 4, EIGHTH, 256), BF16),
        ((2, 4, EIGHTH, 256), BF16),
        ((2, 2, QUARTER, 128), BF16),
        ((2, QUARTER, 128), BF16),
        ((4, 2, 2, 4, QUARTER, 128), F32),
        ((4, 2, 4, QUARTER, 128), F32),
        ((2, 4, 2, 2, QUARTER, 128), BF16),
        ((2, 5, 2, 2, QUARTER, 128), BF16),
        ((4, QUARTER, 128), BF16),
        ((4, QUARTER, 128), BF16),
    ]
    grads = pl.pallas_call(
        kernel,
        out_shape=pltpu.VMEM((2, 768, 128), BF16),
        in_specs=[pl.BlockSpec(memory_space=pl.ANY)] * 3,
        out_specs=vmem,
        scratch_shapes=[pltpu.VMEM(s, t) for s, t in shapes]
        + [pltpu.SemaphoreType.DMA((n,)) for n in (DEPARTURES, ARRIVALS, 3)],
        compiler_params=pltpu.CompilerParams(
            collective_id=0, has_side_effects=True, vmem_limit_bytes=62 * 2**20
        ),
    )(queries.reshape(4, QUARTER, 128), passages, positive.reshape(6, 128))
    return grads[0], grads[1]


def solution(mesh):
    finer = Mesh(mesh.devices.reshape(4, 4, 2, 2, 4), ("zl", "x", "c", "zh", "y"))
    dp, mp = ("zl", "x", "c"), ("zh", "y")
    return jax.shard_map(
        local,
        mesh=finer,
        in_specs=(P(dp, mp), P(dp, mp), P(dp)),
        out_specs=(P(dp, mp), P(dp, mp)),
        check_vma=False,
    )
```

```python
import functools
import math

import jax
import jax.numpy as jnp
from jax import lax
from jax.experimental import pallas as pl
from jax.experimental.pallas import tpu as pltpu
from jax.sharding import Mesh
from jax.sharding import PartitionSpec as P

BF16, F32 = jnp.bfloat16, jnp.float32
D = 1024
SCALE = 3.0 / math.sqrt(D)
EIGHTH, QUARTER, HALF = 96, 192, 384
BLOCK = 1536
GROUP = 768
ARRIVALS, DEPARTURES = 73, 25
NT = (((1,), (1,)), ((), ()))
TN = (((0,), (0,)), ((), ()))


def place(dx=0, dy=0, dz=0, dc=0):
    z = lax.rem(lax.axis_index("zh") * 4 + lax.axis_index("zl") + dz + 8, 8)
    return {
        "zl": lax.rem(z, 4),
        "x": lax.rem(lax.axis_index("x") + dx + 4, 4),
        "c": lax.rem(lax.axis_index("c") + dc, 2),
        "zh": lax.div(z, 4),
        "y": lax.rem(lax.axis_index("y") + dy + 4, 4),
    }


def kernel(
    q_hbm, p_hbm, pos_hbm, out,
    q, p, pos, qb, pb, posb, sc, sg, st,
    da, db, own_a, own_b, ra, rb, s2a, s2b, r2a, r2b, zs, zr,
    dps, dpr, sf, rf, sy, ry,
    ssem, rsem, isem,
):
    x, y, c, zl, zh = (lax.axis_index(a) for a in ("x", "y", "c", "zl", "zh"))
    oc = 1 - c
    oz = 1 - zh
    arrivals, departures, leaving = {}, {}, {}

    def send(src, dst, tag, out=None, **where):
        out = tag if out is None else out
        copy = pltpu.make_async_remote_copy(
            src_ref=src, dst_ref=dst,
            send_sem=ssem.at[departures.setdefault(out, len(departures))],
            recv_sem=rsem.at[arrivals.setdefault(tag, len(arrivals))],
            device_id=place(**where), device_id_type=pl.DeviceIdType.MESH,
        )
        copy.start()
        leaving.setdefault(out, []).append(dst)

    def arrived(tag, ref):
        pltpu.make_async_copy(ref, ref, rsem.at[arrivals[tag]]).wait()

    def left(out, ref):
        pltpu.make_async_copy(ref, ref, ssem.at[departures[out]]).wait()

    def half_of(dz):
        return lax.div(lax.rem(zh * 4 + zl + dz, 8), 4)

    plane = [(dx, dy) for dx in range(4) for dy in range(4) if dx or dy]
    peers = [dict(dx=dx, dy=dy) for dx, dy in plane]
    peers += [dict(dz=1), dict(dz=-1), dict(dz=4), dict(dc=1)]
    inputs = [
        pltpu.make_async_copy(a, b, isem.at[k]) for k, (a, b) in enumerate(((q_hbm, q), (p_hbm, p), (pos_hbm, pos)))
    ]
    for copy in inputs:
        copy.start()
    barrier = pltpu.get_barrier_semaphore()
    for where in peers:
        pl.semaphore_signal(barrier, inc=1, device_id=place(**where), device_id_type=pl.DeviceIdType.MESH)
    pl.semaphore_wait(barrier, len(peers))

    for copy in inputs:
        copy.wait()

    mine = pl.ds(pl.multiple_of(c * QUARTER, 16), QUARTER)
    send(q.at[pl.ds(oz * 2, 2)], qb.at[0, zh, :, pl.ds(0, QUARTER)], "swap", dz=4)
    for d in (1, 3, 2):
        rows = pl.ds(pl.multiple_of(lax.rem(y + d, 4) * QUARTER, 16), QUARTER)
        send(p.at[rows], pb.at[-d % 4, zh, mine], ("spread", -d % 4), "spread", dy=d)

    def share(src, h, tag):
        for d in (1, 3, 2):
            send(src, qb.at[-d % 4, h, :, pl.ds(0, QUARTER)], ("y", -d % 4, tag), ("share", tag), dy=d)
            send(src, qb.at[0, h, :, pl.ds((-d % 4) * QUARTER, QUARTER)], ("x", -d % 4, tag), ("share", tag), dx=d)

    share(q.at[pl.ds(zh * 2, 2)], zh, 0)
    for d in (1, 3, 2):
        send(pos, posb.at[-d % 4], "pos", dx=d)
    for g in (0, 1):
        qb[0, zh, g, 0:QUARTER, :] = q[zh * 2 + g]
    posb[0] = pos[...]
    pb[0, zh, mine, :] = p[pl.ds(pl.multiple_of(y * QUARTER, 16), QUARTER), :]

    def piece(dz, sub):
        rows = pl.ds(pl.multiple_of((dz % 4) * 2 * QUARTER + c * QUARTER, 16), QUARTER)
        ys = pl.ds(0, 4) if sub is None else pl.ds(sub * 2, 2)
        return ys, half_of(dz), rows

    def pass_on(dz, sub, step):
        ys, h, rows = piece(dz, sub)
        to = (dz - step) % 8
        to_rows = pl.ds(pl.multiple_of((to % 4) * 2 * QUARTER + c * QUARTER, 16), QUARTER)
        send(pb.at[ys, h, rows], pb.at[ys, h, to_rows], ("ring", to, sub), "ring", dz=step)

    def ring_arrived(dz, sub):
        arrived(("ring", dz, sub), pb.at[pl.ds(0, 2), 0, pl.ds(0, QUARTER)])

    def to_core(dz):
        ys, h, rows = piece(dz, None)
        send(pb.at[ys, h, rows], pb.at[ys, h, rows], ("core", dz), "core", dc=1)

    def core_arrived(*dzs):
        for dz in dzs:
            arrived(("core", dz), pb.at[:, 0, pl.ds(0, QUARTER)])

    def spread_arrived(*ds):
        for d in ds:
            arrived(("spread", d), pb.at[0, 0, pl.ds(0, QUARTER)])

    def groups_of(groups):
        return pl.ds(0, 2) if groups == "both" else pl.ds(groups, 1)

    def spread_y(k, tag, h, groups):
        gs, rows = groups_of(groups), pl.ds(0, EIGHTH)
        for d in (1, 3, 2):
            to_rows = pl.ds((-d % 4) * QUARTER, EIGHTH)
            send(qb.at[k, h, gs, rows], qb.at[k, h, gs, to_rows], ("second", tag, groups), dx=d)

    def spread_x(k, tag, h, groups):
        gs, rows = groups_of(groups), pl.ds(k * QUARTER + EIGHTH, EIGHTH)
        for d in (1, 3, 2):
            send(qb.at[0, h, gs, rows], qb.at[-d % 4, h, gs, rows], ("second", tag, groups), dy=d)

    def share_arrived(way, k, tag):
        arrived((way, k, tag), qb.at[0, 0, :, pl.ds(0, QUARTER)])

    def second_arrived(tag, groups):
        arrived(("second", tag, groups), qb.at[pl.ds(0, 3), 0, groups_of(groups), pl.ds(0, 576)])

    def hop(n):
        for sub in (0, 1):
            for dz, step in ((n, -1), (8 - n, 1)):
                ring_arrived(dz, sub)
                if n < 3 or (sub == 0) == (step == -1):
                    pass_on(dz, sub, step)
        to_core(n)
        to_core(8 - n)

    spread_arrived(1)
    pass_on(0, 0, 1)
    pass_on(0, 0, -1)
    spread_arrived(3, 2)
    pass_on(0, 1, 1)
    pass_on(0, 1, -1)
    to_core(0)
    share_arrived("x", 1, 0)
    spread_x(1, 0, zh, "both")
    share_arrived("y", 1, 0)
    spread_y(1, 0, zh, "both")
    arrived("swap", qb.at[0, 0, :, pl.ds(0, QUARTER)])
    share(qb.at[0, oz, :, pl.ds(0, QUARTER)], oz, 1)
    for k in (3, 2):
        share_arrived("x", k, 0)
        spread_x(k, 0, zh, "both")
        share_arrived("y", k, 0)
        spread_y(k, 0, zh, "both")
    hop(1)
    hop(2)
    for k in (1, 3, 2):
        share_arrived("x", k, 1)
        share_arrived("y", k, 1)
    for g in (0, 1):
        for k in (1, 3, 2):
            spread_x(k, 1, oz, g)
            spread_y(k, 1, oz, g)
    hop(3)
    arrived("pos", posb.at[pl.ds(1, 3)])
    second_arrived(0, "both")
    second_arrived(1, 0)

    def wide(ref, *at):
        return jnp.concatenate([ref[(k, h, *at)] for k in range(4) for h in range(2)], axis=1)

    best = {0: None, 1: None}

    def scores(g, n):
        rows = slice(n * HALF, (n + 1) * HALF)
        sc[g, rows, :] = lax.dot_general(wide(pb, rows), wide(qb, g), NT, preferred_element_type=F32) * SCALE

    def tally(g, n):
        s = sc[g, n * HALF : (n + 1) * HALF, :]
        high = jnp.max(s, axis=0, keepdims=True)
        if best[g] is None:
            best[g] = high, jnp.sum(jnp.exp(s - high), axis=0, keepdims=True)
        else:
            top, total = best[g]
            higher = jnp.maximum(top, high)
            total = total * jnp.exp(top - higher) + jnp.sum(jnp.exp(s - higher), axis=0, keepdims=True)
            best[g] = higher, total

    def publish(g):
        top, total = best[g]
        for i in range(4):
            st[g, 0, i, 0:1, :] = top[:, i * QUARTER : (i + 1) * QUARTER]
            st[g, 0, i, 1:2, :] = total[:, i * QUARTER : (i + 1) * QUARTER]
        for dx, dy in plane:
            send(st.at[g, 0], st.at[g, (-dx % 4) * 4 + (-dy % 4)], ("stats", g), dx=dx, dy=dy)

    core_arrived(2, 6)
    scores(0, 2)
    for sub in (0, 1):
        ring_arrived(4, sub)
    to_core(4)
    core_arrived(1, 5, 3, 7)
    scores(0, 1)
    tally(0, 2)
    scores(0, 3)
    tally(0, 1)
    tally(0, 3)
    core_arrived(0, 4)
    scores(0, 0)
    tally(0, 0)
    publish(0)
    second_arrived(1, 1)
    scores(1, 2)
    scores(1, 1)
    tally(1, 2)
    scores(1, 3)
    tally(1, 1)
    scores(1, 0)
    tally(1, 3)
    tally(1, 0)
    publish(1)

    logs_of, targets_of = {}, {}

    def normaliser(g):
        arrived(("stats", g), st.at[g, pl.ds(1, 15)])
        logs = []
        for i in range(4):
            pairs = [(k, (i - k // 4) % 4) for k in range(16)]
            tops = [st[g, k, n, 0:1, :] for k, n in pairs]
            high = functools.reduce(jnp.maximum, tops)
            total = sum(st[g, k, n, 1:2, :] * jnp.exp(t - high) for (k, n), t in zip(pairs, tops))
            logs.append(high + jnp.log(total))
        targets = []
        for i in range(4):
            three = jnp.concatenate([posb[i, pl.ds(zh * 3 + t, 1), :] for t in range(3)], axis=1)
            targets.append(three[:, g * QUARTER : (g + 1) * QUARTER])
        for half in (0, 1):
            two = slice(half * 2, half * 2 + 2)
            logs_of[g, half] = jnp.concatenate(logs[two], axis=1)
            targets_of[g, half] = jnp.concatenate(targets[two], axis=1)

    def normalise(g, half):
        columns = slice(half * HALF, (half + 1) * HALF)
        log_total, targets = logs_of[g, half], targets_of[g, half]

        def normal(j, carry):
            rows = pl.ds(pl.multiple_of(j * QUARTER, 16), QUARTER)
            owner = (lax.rem(zl + lax.div(j, 2), 4) * 4 + x) * 2 + lax.rem(j, 2)
            ids = lax.broadcasted_iota(jnp.int32, (QUARTER, HALF), 0) + (owner * 768 + y * QUARTER)
            e = jnp.exp(sc[g, rows, columns] - log_total)
            sg[g, rows, columns] = jnp.where(ids == targets, e - 1.0, e).astype(BF16)
            return carry

        lax.fori_loop(0, 8, normal, 0)

    def query_gradients(g, half):
        r = lax.dot_general(
            sg[g, :, half * HALF : (half + 1) * HALF], wide(pb), TN, preferred_element_type=F32
        )
        pair = pl.ds(half * 2, 2)
        for k in (1, 3, 2, 0):
            columns = slice(k * 256, (k + 1) * 256)
            for i in range(2):
                part_a = r[i * QUARTER : i * QUARTER + EIGHTH, columns]
                part_b = r[i * QUARTER + EIGHTH : (i + 1) * QUARTER, columns]
                if half or i:
                    da[g, half * 2 + i, k] = part_a.astype(BF16)
                else:
                    own_a[g, k] = part_a
                if k:
                    db[g, k, half * 2 + i] = part_b.astype(BF16)
                else:
                    own_b[g, half * 2 + i] = part_b
            if k:
                send(db.at[g, k, pair], rb.at[g, -k % 4, pair], ("b", g), dy=k)
        for i in (3, 2) if half else (1,):
            send(da.at[g, i], ra.at[g, -i % 4], ("a", g), dx=i)

    def passages(s):
        rows = slice(s * HALF, (s + 1) * HALF)
        r = jnp.dot(
            jnp.concatenate([sg[g, rows, :] for g in range(2)], axis=1),
            jnp.concatenate([wide(qb, g) for g in range(2)], axis=0),
            preferred_element_type=F32,
        )
        for k in range(4):
            for i in range(2):
                for h in range(2):
                    column = k * 256 + h * 128
                    dps[s, i, h, k] = r[i * QUARTER : (i + 1) * QUARTER, column : column + 128]
        send(dps.at[s, oc], dpr.at[s], ("half", s), "half", dc=1)

    def half_arrived(*ss):
        for s in ss:
            arrived(("half", s), dpr.at[s])

    def both(dz, k):
        h = half_of(dz)
        return dps[dz % 4, c, h, k] + dpr[dz % 4, h, k]

    def add_on(way, n, sub, first=False):
        dz = (4 - n) if way == 0 else (4 + n)
        for i in range(2):
            v = both(dz, sub * 2 + i)
            if not first:
                v = v + rf[way, n, sub, i].astype(F32)
            sf[way, n, sub, i] = v.astype(BF16)
        send(sf.at[way, n, sub], rf.at[way, n + 1, sub], ("sum", way, n + 1, sub), "sum", dz=1 - 2 * way)

    def sum_arrived(way, n, sub):
        arrived(("sum", way, n, sub), rf.at[way, n, sub])

    def step(n):
        for way, sub in ((0, 1), (1, 0), (0, 0), (1, 1)):
            sum_arrived(way, n, sub)
            add_on(way, n, sub)

    def second_stage(g):
        arrived(("a", g), ra.at[g, pl.ds(1, 3)])
        arrived(("b", g), rb.at[g, pl.ds(1, 3)])
        for k in (1, 3, 2, 0):
            va = own_a[g, k] + sum(ra[g, i, k].astype(F32) for i in (1, 2, 3))
            vb = own_b[g, k] + sum(rb[g, i, k].astype(F32) for i in (1, 2, 3))
            if k:
                s2a[g, k] = va.astype(BF16)
                send(s2a.at[g, k], r2a.at[g, -k % 4], ("a2", g), dy=k)
                s2b[g, k] = vb.astype(BF16)
                send(s2b.at[g, k], r2b.at[g, -k % 4], ("b2", g), dx=k)
            else:
                own_a[g, 0] = va
                own_b[g, 0] = vb

    def third_stage(g):
        arrived(("a2", g), r2a.at[g, pl.ds(1, 3)])
        arrived(("b2", g), r2b.at[g, pl.ds(1, 3)])
        fa = own_a[g, 0] + sum(r2a[g, k].astype(F32) for k in (1, 2, 3))
        fb = own_b[g, 0] + sum(r2b[g, k].astype(F32) for k in (1, 2, 3))
        for h in range(2):
            zs[h, g, 0:EIGHTH, :] = fa[:, h * 128 : (h + 1) * 128].astype(BF16)
            zs[h, g, EIGHTH:QUARTER, :] = fb[:, h * 128 : (h + 1) * 128].astype(BF16)
        send(zs.at[oz, g], zr.at[g], ("last", g), dz=4)
        out[0, pl.ds(pl.multiple_of(zh * HALF + g * QUARTER, 16), QUARTER), :] = zs[zh, g]

    normaliser(0)
    normalise(0, 1)
    query_gradients(0, 1)
    normalise(0, 0)
    normaliser(1)
    normalise(1, 1)
    normalise(1, 0)
    passages(0)
    query_gradients(0, 0)
    passages(3)
    half_arrived(0)
    add_on(0, 0, 0, True)
    add_on(1, 0, 1, True)
    passages(1)
    query_gradients(1, 1)
    half_arrived(3, 1)
    add_on(0, 1, 1, True)
    add_on(1, 1, 0, True)
    passages(2)
    for way, sub in ((0, 0), (1, 1)):
        sum_arrived(way, 1, sub)
        add_on(way, 1, sub)
    query_gradients(1, 0)
    second_stage(0)
    half_arrived(2)
    step(2)
    step(3)
    second_stage(1)
    third_stage(0)
    third_stage(1)

    def last_step(k):
        v = both(0, k) + rf[0, 4, k // 2, k % 2].astype(F32) + rf[1, 4, k // 2, k % 2].astype(F32)
        if k:
            sy[k] = v.astype(BF16)
            send(sy.at[k], ry.at[-k % 4], "widths", dy=k)
        else:
            out[1, pl.ds(pl.multiple_of(y * QUARTER, 16), QUARTER), :] = v.astype(BF16)

    for way, sub in ((0, 1), (1, 0), (0, 0)):
        sum_arrived(way, 4, sub)
    last_step(1)
    sum_arrived(1, 4, 1)
    for k in (3, 2, 0):
        last_step(k)
    arrived("widths", ry.at[pl.ds(1, 3)])
    for k in (1, 2, 3):
        out[1, pl.ds(pl.multiple_of(lax.rem(y + k, 4) * QUARTER, 16), QUARTER), :] = ry[k]
    for g in (0, 1):
        arrived(("last", g), zr.at[g])
        out[0, pl.ds(pl.multiple_of(oz * HALF + g * QUARTER, 16), QUARTER), :] = zr[g]
    rest = {
        "spread": pb.at[pl.ds(0, 3), 0, pl.ds(0, QUARTER)],
        "ring": pb.at[:, 0, pl.ds(0, 1344)],
        "core": pb.at[:, 0],
        ("share", 0): qb.at[pl.ds(0, 3), 0, 0],
        ("share", 1): qb.at[pl.ds(0, 3), 0, 0],
        "pos": posb.at[pl.ds(1, 3)],
        ("second", 0, "both"): qb.at[pl.ds(0, 3), 0, :, pl.ds(0, 576)],
        ("second", 1, 0): qb.at[pl.ds(0, 3), 0, pl.ds(0, 1), pl.ds(0, 576)],
        ("second", 1, 1): qb.at[pl.ds(0, 3), 0, pl.ds(0, 1), pl.ds(0, 576)],
        "half": dpr,
        "sum": pb.at[:, 0, pl.ds(0, 1344)],
        "widths": ry.at[pl.ds(1, 3)],
    }
    for g in (0, 1):
        rest["stats", g] = st.at[g, pl.ds(1, 15)]
        rest["a", g], rest["b", g] = ra.at[g, pl.ds(1, 3)], rb.at[g, pl.ds(1, 3)]
        rest["a2", g], rest["b2", g] = r2a.at[g, pl.ds(1, 3)], r2b.at[g, pl.ds(1, 3)]
    for out, dsts in leaving.items():
        ref = dsts[0] if len(dsts) == 1 else rest[out]
        size = lambda r: math.prod(r.shape) * r.dtype.itemsize
        assert size(ref) == sum(size(d) for d in dsts), out
        left(out, ref)
    assert (len(arrivals), len(departures)) == (ARRIVALS, DEPARTURES), (len(arrivals), len(departures))


def local(queries, passages, positive):
    vmem = pl.BlockSpec(memory_space=pltpu.VMEM)
    shapes = [
        ((4, QUARTER, 128), BF16),
        ((768, 128), BF16),
        ((6, 128), jnp.int32),
        ((4, 2, 2, GROUP, 128), BF16),
        ((4, 2, BLOCK, 128), BF16),
        ((4, 6, 128), jnp.int32),
        ((2, BLOCK, GROUP), F32),
        ((2, BLOCK, GROUP), BF16),
        ((2, 16, 4, 2, QUARTER), F32),
        ((2, 4, 4, EIGHTH, 256), BF16),
        ((2, 4, 4, EIGHTH, 256), BF16),
        ((2, 4, EIGHTH, 256), F32),
        ((2, 4, EIGHTH, 256), F32),
        ((2, 4, 4, EIGHTH, 256), BF16),
        ((2, 4, 4, EIGHTH, 256), BF16),
        ((2, 4, EIGHTH, 256), BF16),
        ((2, 4, EIGHTH, 256), BF16),
        ((2, 4, EIGHTH, 256), BF16),
        ((2, 4, EIGHTH, 256), BF16),
        ((2, 2, QUARTER, 128), BF16),
        ((2, QUARTER, 128), BF16),
        ((4, 2, 2, 4, QUARTER, 128), F32),
        ((4, 2, 4, QUARTER, 128), F32),
        ((2, 4, 2, 2, QUARTER, 128), BF16),
        ((2, 5, 2, 2, QUARTER, 128), BF16),
        ((4, QUARTER, 128), BF16),
        ((4, QUARTER, 128), BF16),
    ]
    grads = pl.pallas_call(
        kernel,
        out_shape=pltpu.VMEM((2, 768, 128), BF16),
        in_specs=[pl.BlockSpec(memory_space=pl.ANY)] * 3,
        out_specs=vmem,
        scratch_shapes=[pltpu.VMEM(s, t) for s, t in shapes]
        + [pltpu.SemaphoreType.DMA((n,)) for n in (DEPARTURES, ARRIVALS, 3)],
        compiler_params=pltpu.CompilerParams(
            collective_id=0, has_side_effects=True, vmem_limit_bytes=62 * 2**20
        ),
    )(queries.reshape(4, QUARTER, 128), passages, positive.reshape(6, 128))
    return grads[0], grads[1]


def solution(mesh):
    finer = Mesh(mesh.devices.reshape(4, 4, 2, 2, 4), ("zl", "x", "c", "zh", "y"))
    dp, mp = ("zl", "x", "c"), ("zh", "y")
    return jax.shard_map(
        local,
        mesh=finer,
        in_specs=(P(dp, mp), P(dp, mp), P(dp)),
        out_specs=(P(dp, mp), P(dp, mp)),
        check_vma=False,
    )
```
